32 devices in a mesh: ba: 4 (over x, core), ma: 4 (over z), row: 2 (over y).
Axes of the slice: x: 2, y: 2, z: 4, core: 2. Of those that a mesh axis runs over, the one named last changes fastest.
Arguments:
- tokens: bfloat16 [8, 256, 4096], P(('ba', 'row'), None, 'ma'), may hold values from -6 to 6
- attn_gain: bfloat16 [4096], P('ma'), may hold values from 0.25 to 1.75
- query_weight: bfloat16 [4096, 4096], P('row', 'ma'), may hold values from -0.046875 to 0.046875
- key_weight: bfloat16 [4096, 4096], P('row', 'ma'), may hold values from -0.046875 to 0.046875
- value_projection_matrix: bfloat16 [4096, 4096], P('row', 'ma'), may hold values from -0.09375 to 0.09375
- attention_output_matrix: bfloat16 [4096, 4096], P('ma', 'row'), may hold values from -0.125 to 0.125
- bucket_bias_matrix: float32 [32, 64], P(None, 'ma'), may hold values from -6 to 215, as said below
- ffn_gain: bfloat16 [4096], P('ma'), may hold values from 0.25 to 1.75
- gate_weight: bfloat16 [4096, 8192], P(None, ('ma', 'row')), may hold values from -0.09375 to 0.09375
- up_weight: bfloat16 [4096, 8192], P(None, ('ma', 'row')), may hold values from -0.09375 to 0.09375
- down_projection_weight: bfloat16 [8192, 4096], P(('ma', 'row')), may hold values from -0.09375 to 0.09375
Outputs:
- encoded: bfloat16 [8, 256, 4096], P(('ba', 'row'), None, 'ma')
The draws below stay inside these ranges and needn't reach their ends.
Inputs may be any that keep to these rules, and one draw needn't show every extreme that they name: `bucket_bias_matrix`: entries of the relative position table.
All inputs are finite; a program needn't handle non-finite values.
Results may differ from the reference program's by a relative error of at most 0.017.
Values may be sent and summed in bfloat16 or wider, within the bound.
A program may use at most 128 MiB of HBM per device.

```python
import jax
import jax.numpy as jnp
from jax import lax

D = 4096
H = 64
DH = 64
FF = 8192
BUCKETS = 32
LEN = 256
BATCH = 8
N_MA = 4


def draw_bucket_bias_matrix(key, part):
    first_key, second_key = jax.random.split(key)
    normal_part = jnp.clip(jax.random.normal(first_key, (BUCKETS, H), jnp.float32), -6.0, 6.0)
    return normal_part


def spiked(entries, own_key, source, target, shards_of, factor):
    owner, partner = [(jnp.arange(entries.shape[axis_at]) // (entries.shape[axis_at] // shards_of)).reshape([-1 if axis == axis_at else 1 for axis in range(entries.ndim)]) for axis_at in (source, target)]
    chosen = jax.random.permutation(own_key, shards_of)[partner]
    strong = (owner == chosen) | (owner == (partner + shards_of // 2) % shards_of)
    return jnp.where(strong, factor * entries, entries)


def steps_of(stream_key, shape, cuts, smallest, largest):
    def one(position, shards_of):
        heights = jax.random.uniform(jax.random.fold_in(jax.random.fold_in(stream_key, 6), position), (shards_of,), jnp.float32, smallest / len(cuts), largest / len(cuts))
        return jnp.repeat(jnp.exp(heights), shape[position] // shards_of).reshape((-1,) + (1,) * (len(shape) - position - 1))

    loudness = one(*cuts[0])
    for cut in cuts[1:]:
        loudness = loudness * one(*cut)
    return loudness


def noise(stream_key, extent, spread, limit, cuts=(), held_as=jnp.bfloat16):
    loudness = steps_of(stream_key, extent, cuts, -0.22, 0.18) if cuts else 1.0
    entries = jax.random.normal(stream_key, extent, jnp.float32) * spread * loudness
    return jnp.minimum(jnp.maximum(entries, -limit), limit).astype(held_as)


def noise_with(rng, dims, deviation, most, pieces, heavy, kind=jnp.bfloat16):
    result = deviation * jax.random.normal(rng, dims, jnp.float32)
    if pieces:
        result = result * steps_of(rng, dims, pieces, -0.22, 0.18)
    return jnp.clip(spiked(result, jax.random.fold_in(rng, 3), *heavy), -most, most).astype(kind)


def setup_inputs(seed: int = 0) -> dict:
    key_of = jax.random.split(jax.random.key(seed), 12)
    tokens = noise(key_of[0], (BATCH, LEN, D), 1.0, 6.0, ((0, 8), (2, 4)))
    attn_gain = jnp.clip(1.0 + 0.15 * jax.random.normal(key_of[1], (D,), jnp.float32), 0.25, 1.75).astype(jnp.bfloat16)
    query_weight = noise(key_of[2], (D, H * DH), (4 * D) ** -0.5, 0.046875, ((0, 2), (1, 4)))
    key_weight = noise(key_of[3], (D, H * DH), (4 * D) ** -0.5, 0.046875, ((0, 2), (1, 4)))
    value_projection_matrix = noise(key_of[4], (D, H * DH), D ** -0.5, 0.09375, ((0, 2), (1, 4)))
    attention_output_matrix = noise_with(key_of[5], (H * DH, D), (H * DH) ** -0.5, 0.125, ((0, 4), (1, 2)), (0, 1, 4, 2.0))
    bucket_bias_matrix = draw_bucket_bias_matrix(jax.random.fold_in(key_of[11], 71), 0)
    ffn_gain = jnp.clip(1.0 + 0.15 * jax.random.normal(key_of[7], (D,), jnp.float32), 0.25, 1.75).astype(jnp.bfloat16)
    gate_weight = noise(key_of[8], (D, FF), D ** -0.5, 0.09375, ((1, 8),))
    up_weight = noise(key_of[9], (D, FF), D ** -0.5, 0.09375, ((1, 8),))
    down_projection_weight = noise_with(key_of[10], (FF, D), FF ** -0.5, 0.09375, ((0, 8),), (0, 1, 8, 2.0))
    return dict(tokens=tokens, attn_gain=attn_gain, query_weight=query_weight, key_weight=key_weight, value_projection_matrix=value_projection_matrix, attention_output_matrix=attention_output_matrix, bucket_bias_matrix=bucket_bias_matrix, ffn_gain=ffn_gain, gate_weight=gate_weight, up_weight=up_weight, down_projection_weight=down_projection_weight)


bucket_thresholds = (1, 2, 3, 4, 5, 6, 7, 8, 11, 16, 23, 32, 45, 64, 91, 128)
epsilon = 1e-06

def buckets(length):
    places = jnp.arange(length, dtype=jnp.int32)
    offset = places[None, :] - places[:, None]
    distance = jnp.abs(offset)
    backward = jnp.zeros_like(distance)
    for threshold in bucket_thresholds[:15]:
        backward = backward + (distance >= threshold).astype(jnp.int32)
    forward = jnp.full_like(distance, 15)
    for threshold in bucket_thresholds:
        forward = forward + (distance >= threshold).astype(jnp.int32)
    return jnp.where(offset > 0, forward, backward)

def rms_scale(values, gain):
    mean_square = lax.optimization_barrier(jnp.mean(values * values, axis=-1, keepdims=True))
    return (values * lax.rsqrt(mean_square + epsilon) * gain.astype(jnp.float32)).astype(jnp.bfloat16)

def grouped_sum(left, right, groups):
    span = left.shape[1] // groups

    def add_group(running, group_index):
        columns = lax.dynamic_slice_in_dim(left, group_index * span, span, 1)
        matrix = lax.dynamic_slice_in_dim(right, group_index * span, span, 0)
        partial_term = jnp.dot(columns, matrix, preferred_element_type=jnp.float32).astype(jnp.bfloat16)
        partial_term = lax.optimization_barrier(partial_term).astype(jnp.float32)
        return (running + partial_term, None)
    start_sum = jnp.zeros((left.shape[0], right.shape[1]), jnp.float32)
    total, unused = lax.scan(add_group, start_sum, jnp.arange(groups, dtype=jnp.int32))
    return total

def reference(tokens, attn_gain, query_weight, key_weight, value_projection_matrix, attention_output_matrix, bucket_bias_matrix, ffn_gain, gate_weight, up_weight, down_projection_weight):
    batch_size, length, model_width = tokens.shape
    head_count = bucket_bias_matrix.shape[1]
    inner_width = query_weight.shape[1]
    head_size = inner_width // head_count
    token_rows = tokens.reshape(batch_size * length, model_width).astype(jnp.float32)
    normed = rms_scale(token_rows, attn_gain)
    projected = tuple((jnp.dot(normed, matrix, preferred_element_type=jnp.float32).astype(jnp.bfloat16).reshape(batch_size, length, head_count, head_size) for matrix in (query_weight, key_weight, value_projection_matrix)))
    relative_position_scores = jnp.transpose(bucket_bias_matrix[buckets(length)], (2, 0, 1))

    def attend(inputs):
        query_heads, key_heads, value_heads = inputs
        scores = jnp.einsum('qhd,khd->hqk', query_heads.astype(jnp.float32), key_heads.astype(jnp.float32)) + relative_position_scores
        row_max = lax.optimization_barrier(jnp.max(scores, axis=-1, keepdims=True))
        exponent = jnp.exp(scores - row_max)
        weights = (exponent / lax.optimization_barrier(jnp.sum(exponent, axis=-1, keepdims=True))).astype(jnp.bfloat16)
        return jnp.einsum('hqk,khd->qhd', weights.astype(jnp.float32), value_heads.astype(jnp.float32)).astype(jnp.bfloat16)
    attended = lax.map(attend, projected).reshape(batch_size * length, inner_width)
    attn_out = grouped_sum(attended, attention_output_matrix, N_MA)
    residual_stream = (token_rows + attn_out).astype(jnp.bfloat16)
    residual_f = residual_stream.astype(jnp.float32)
    ffn_in = rms_scale(residual_f, ffn_gain)
    gate_act = jnp.dot(ffn_in, gate_weight, preferred_element_type=jnp.float32)
    up_act = jnp.dot(ffn_in, up_weight, preferred_element_type=jnp.float32)
    hidden = (jax.nn.gelu(gate_act, approximate=True) * up_act).astype(jnp.bfloat16)
    ffn_out = jnp.dot(hidden, down_projection_weight, preferred_element_type=jnp.float32)
    encoded = (residual_f + ffn_out).astype(jnp.bfloat16)
    return encoded.reshape(batch_size, length, model_width)
```

```python
import functools

import jax
import jax.numpy as jnp
from jax import lax
from jax.experimental import pallas as pl
from jax.experimental.pallas import tpu as pltpu
from jax.sharding import PartitionSpec as P

bucket_thresholds = (1, 2, 3, 4, 5, 6, 7, 8, 11, 16, 23, 32, 45, 64, 91, 128)
epsilon = 1e-06


def buckets(length):
    places = jnp.arange(length, dtype=jnp.int32)
    offset = places[None, :] - places[:, None]
    distance = jnp.abs(offset)
    backward = jnp.zeros_like(distance)
    for threshold in bucket_thresholds[:15]:
        backward = backward + (distance >= threshold).astype(jnp.int32)
    forward = jnp.full_like(distance, 15)
    for threshold in bucket_thresholds:
        forward = forward + (distance >= threshold).astype(jnp.int32)
    return jnp.where(offset > 0, forward, backward)


def rms_scale(values, gain):
    mean_square = jnp.mean(values * values, axis=-1, keepdims=True)
    return (values * lax.rsqrt(mean_square + epsilon) * gain.astype(jnp.float32)).astype(
        jnp.bfloat16
    )


MESH = pl.DeviceIdType.MESH


def greet(me, count, row):
    barrier = pltpu.get_barrier_semaphore()

    @pl.when(me > 0)
    def _():
        pl.semaphore_signal(barrier, inc=1, device_id={"ma": me - 1}, device_id_type=MESH)

    @pl.when(me < count - 1)
    def _():
        pl.semaphore_signal(barrier, inc=1, device_id={"ma": me + 1}, device_id_type=MESH)

    pl.semaphore_signal(barrier, inc=1, device_id={"row": 1 - row}, device_id_type=MESH)
    inner = jnp.logical_and(me > 0, me < count - 1)
    pl.semaphore_wait(barrier, jnp.where(inner, 3, 2))


def gather_kernel(count, cuts, halved, x_ref, out_ref, local_sem, send_sem, z_sem, y_sem):
    me = lax.axis_index("ma")
    row = lax.axis_index("row")
    length, width = x_ref.shape
    pieces = len(cuts) - 1
    greet(me, count, row)

    def leaves(block):
        return block // (count // 2) == 1 - row if halved else block >= 0

    def comes(block):
        return block // (count // 2) == row if halved else block >= 0

    def place(block, piece, which):
        return out_ref.at[
            pl.ds(pl.multiple_of(which * length + cuts[piece], 16), cuts[piece + 1] - cuts[piece]),
            pl.ds(pl.multiple_of(block * width, width), width),
        ]

    def copy(way, block, piece, src=None):
        here = place(block, piece, row)
        target = ({"ma": me + 1}, {"ma": me - 1}, {"row": 1 - row})[way]
        sem = y_sem if way == 2 else z_sem
        return pltpu.make_async_remote_copy(
            src_ref=here if src is None else src,
            dst_ref=here,
            send_sem=send_sem.at[way, block, piece],
            recv_sem=sem.at[block, piece],
            device_id=target,
            device_id_type=MESH,
        )

    def own(piece):
        return x_ref.at[pl.ds(cuts[piece], cuts[piece + 1] - cuts[piece]), :]

    for piece in range(pieces):

        @pl.when(me < count - 1)
        def _():
            copy(0, me, piece, own(piece)).start()

        @pl.when(me > 0)
        def _():
            copy(1, me, piece, own(piece)).start()

        @pl.when(leaves(me))
        def _():
            copy(2, me, piece, own(piece)).start()

    mine = pltpu.make_async_copy(
        x_ref,
        out_ref.at[
            pl.ds(pl.multiple_of(row * length, length), length),
            pl.ds(pl.multiple_of(me * width, width), width),
        ],
        local_sem,
    )
    mine.start()
    for step in range(1, count):
        for piece in range(pieces):

            @pl.when(me - step >= 0)
            def _():
                block = me - step
                copy(0, block, piece).wait_recv()

                @pl.when(me < count - 1)
                def _():
                    copy(0, block, piece).start()

                @pl.when(leaves(block))
                def _():
                    copy(2, block, piece).start()

            @pl.when(me + step < count)
            def _():
                block = me + step
                copy(1, block, piece).wait_recv()

                @pl.when(me > 0)
                def _():
                    copy(1, block, piece).start()

                @pl.when(leaves(block))
                def _():
                    copy(2, block, piece).start()

    mine.wait()
    for block in range(count):
        for piece in range(pieces):
            here = place(block, piece, 1 - row)
            arrival = pltpu.make_async_remote_copy(
                src_ref=here,
                dst_ref=here,
                send_sem=send_sem.at[2, block, piece],
                recv_sem=y_sem.at[block, piece],
                device_id={"row": 1 - row},
                device_id_type=MESH,
            )

            @pl.when(comes(jnp.int32(block)))
            def _():
                arrival.wait_recv()

            @pl.when(leaves(jnp.int32(block)))
            def _():
                copy(2, block, piece).wait_send()

            @pl.when(jnp.logical_and(me < count - 1, block <= me))
            def _():
                copy(0, block, piece).wait_send()

            @pl.when(jnp.logical_and(me > 0, block >= me))
            def _():
                copy(1, block, piece).wait_send()


def gather_all(values, count, cuts, halved, collective_id):
    length, width = values.shape
    pieces = len(cuts) - 1
    return pl.pallas_call(
        functools.partial(gather_kernel, count, cuts, halved),
        out_shape=jax.ShapeDtypeStruct((2 * length, count * width), values.dtype),
        in_specs=[pl.BlockSpec(memory_space=pltpu.VMEM)],
        out_specs=pl.BlockSpec(memory_space=pltpu.VMEM),
        scratch_shapes=[
            pltpu.SemaphoreType.DMA,
            pltpu.SemaphoreType.DMA((3, count, pieces)),
            pltpu.SemaphoreType.DMA((count, pieces)),
            pltpu.SemaphoreType.DMA((count, pieces)),
        ],
        compiler_params=pltpu.CompilerParams(collective_id=collective_id, has_side_effects=True),
    )(values)


def reduce_kernel(count, pieces, paired, left_ref, right_ref, out_ref, *scratch):
    if paired:
        sent, landed, y_send, y_recv = scratch[:4]
    total, left_in, right_in, right_out, left_out, r_send, r_recv, l_send, l_recv = scratch[-9:]
    me = lax.axis_index("ma")
    row = lax.axis_index("row")
    length, width = out_ref.shape
    step_rows = length // pieces
    greet(me, count, row)

    def y_copy(unit):
        return pltpu.make_async_remote_copy(
            src_ref=sent.at[unit],
            dst_ref=landed.at[unit],
            send_sem=y_send.at[unit],
            recv_sem=y_recv.at[unit],
            device_id={"row": 1 - row},
            device_id_type=MESH,
        )

    def r_copy(unit):
        return pltpu.make_async_remote_copy(
            src_ref=right_out.at[unit],
            dst_ref=left_in.at[unit],
            send_sem=r_send.at[unit],
            recv_sem=r_recv.at[unit],
            device_id={"ma": me + 1},
            device_id_type=MESH,
        )

    def l_copy(unit):
        return pltpu.make_async_remote_copy(
            src_ref=left_out.at[unit],
            dst_ref=right_in.at[unit],
            send_sem=l_send.at[unit],
            recv_sem=l_recv.at[unit],
            device_id={"ma": me - 1},
            device_id_type=MESH,
        )

    def product(which, block, piece):
        start = pl.multiple_of(which * length + piece * step_rows, step_rows)
        columns = pl.ds(pl.multiple_of(block * width, width), width)
        return jnp.dot(
            left_ref[pl.ds(start, step_rows), :],
            right_ref[:, columns],
            preferred_element_type=jnp.float32,
        )

    def ordered(body):
        def turn(index, carry):
            piece = index % pieces
            side = index // pieces
            step = count - 1 - side // 2
            rightward = side % 2 == 0
            block = jnp.where(rightward, me + step, me - step)
            inside = jnp.logical_and(block >= 0, block < count)

            @pl.when(jnp.logical_and(inside, jnp.logical_or(step > 0, rightward)))
            def _():
                body(block, piece, block * pieces + piece)

            return carry

        lax.fori_loop(0, 2 * count * pieces, turn, 0)

    def send_peer(block, piece, unit):
        sent[unit] = product(1 - row, block, piece).astype(jnp.bfloat16)
        y_copy(unit).start()

    if paired:
        ordered(send_peer)

    def pass_on(block, piece, unit):
        total[...] = product(row if paired else 0, block, piece)
        if paired:
            y_copy(unit).wait_recv()
            total[...] = total[...] + landed[unit].astype(jnp.float32)

        @pl.when(jnp.logical_and(block >= me, me > 0))
        def _():
            r_copy(unit).wait_recv()
            total[...] = total[...] + left_in[unit].astype(jnp.float32)

        @pl.when(jnp.logical_and(block <= me, me < count - 1))
        def _():
            l_copy(unit).wait_recv()
            total[...] = total[...] + right_in[unit].astype(jnp.float32)

        @pl.when(block > me)
        def _():
            right_out[unit] = total[...].astype(jnp.bfloat16)
            r_copy(unit).start()

        @pl.when(block < me)
        def _():
            left_out[unit] = total[...].astype(jnp.bfloat16)
            l_copy(unit).start()

        @pl.when(block == me)
        def _():
            out_ref[pl.ds(pl.multiple_of(piece * step_rows, step_rows), step_rows), :] = total[...]

    ordered(pass_on)

    def drain(unit, carry):
        block = unit // pieces
        if paired:
            y_copy(unit).wait_send()

        @pl.when(block > me)
        def _():
            r_copy(unit).wait_send()

        @pl.when(block < me)
        def _():
            l_copy(unit).wait_send()

        return carry

    lax.fori_loop(0, count * pieces, drain, 0)


def reduce_all(left, right, count, pieces, paired, collective_id):
    length = left.shape[0] // (2 if paired else 1)
    width = right.shape[1] // count
    units = count * pieces
    blocks = pltpu.VMEM((units, length // pieces, width), jnp.bfloat16)
    sems = pltpu.SemaphoreType.DMA((units,))
    return pl.pallas_call(
        functools.partial(reduce_kernel, count, pieces, paired),
        out_shape=jax.ShapeDtypeStruct((length, width), jnp.float32),
        in_specs=[pl.BlockSpec(memory_space=pltpu.VMEM)] * 2,
        out_specs=pl.BlockSpec(memory_space=pltpu.VMEM),
        scratch_shapes=([blocks, blocks, sems, sems] if paired else [])
        + [pltpu.VMEM((length // pieces, width), jnp.float32)]
        + [blocks] * 4
        + [sems] * 4,
        compiler_params=pltpu.CompilerParams(
            collective_id=collective_id, has_side_effects=True, vmem_limit_bytes=60 * 2**20
        ),
    )(left, right)


def front_kernel(
    count,
    chunks,
    groups,
    tok_ref,
    gain_ref,
    table_ref,
    wq_ref,
    wk_ref,
    wv_ref,
    wo_ref,
    att_ref,
    gains_ref,
    out_full_ref,
    xs,
    weights,
    scaled,
    part_out,
    part_in,
    sums_out,
    sums_in,
    bias,
    gain_tile,
    w_sem,
    own_sem,
    gain_sem,
    wo_sem,
    g_send,
    g_recv,
    y_send,
    y_recv,
    z_send,
    z_recv,
    p_send,
    p_recv,
    s_send,
    s_recv,
    wy_send,
    wy_recv,
    wf_send,
    wf_recv,
):
    me = lax.axis_index("ma")
    row = lax.axis_index("row")
    ba = lax.axis_index("ba")
    length, width = tok_ref.shape
    half_blocks = count // 2
    half = half_blocks * width
    inner = att_ref.shape[1]
    heads = table_ref.shape[1]
    head_size = inner // heads
    rows = length // chunks
    group_width = inner // groups
    home = me // half_blocks == row
    col_half = wo_ref.shape[1]
    pieces = wy_send.shape[0]
    lane_rows = wo_ref.shape[0] // 4
    piece_rows = lane_rows // pieces
    lane = ba % 4

    barrier = pltpu.get_barrier_semaphore()

    def hello(offset, carry):
        pl.semaphore_signal(
            barrier, inc=1, device_id={"ma": (me + offset) % count}, device_id_type=MESH
        )
        return carry

    lax.fori_loop(1, count, hello, 0)
    pl.semaphore_signal(barrier, inc=1, device_id={"row": 1 - row}, device_id_type=MESH)
    for flip in (1, 2, 3):
        pl.semaphore_signal(barrier, inc=1, device_id={"ba": ba ^ flip}, device_id_type=MESH)
    pl.semaphore_wait(barrier, count + 3)

    def place(seq, chunk, slot):
        return xs.at[
            seq,
            pl.ds(chunk * rows, rows),
            pl.ds(pl.multiple_of(slot * width, width), width),
        ]

    def z_copy(way, seq, chunk, block, src=None):
        slot = block - row * half_blocks
        here = place(seq, chunk, slot)
        return pltpu.make_async_remote_copy(
            src_ref=here if src is None else src,
            dst_ref=here,
            send_sem=z_send.at[way, seq, chunk, slot],
            recv_sem=z_recv.at[seq, chunk, slot],
            device_id={"ma": me + 1 - 2 * way},
            device_id_type=MESH,
        )

    def own(chunk):
        return tok_ref.at[pl.ds(chunk * rows, rows), :]

    def y_copy(chunk):
        return pltpu.make_async_remote_copy(
            src_ref=own(chunk),
            dst_ref=place(row, chunk, me - (1 - row) * half_blocks),
            send_sem=y_send.at[chunk],
            recv_sem=y_recv.at[chunk],
            device_id={"row": 1 - row},
            device_id_type=MESH,
        )

    def y_arrival(chunk):
        here = place(1 - row, chunk, me - row * half_blocks)
        return pltpu.make_async_remote_copy(
            src_ref=here,
            dst_ref=here,
            send_sem=y_send.at[chunk],
            recv_sem=y_recv.at[chunk],
            device_id={"row": 1 - row},
            device_id_type=MESH,
        )

    def launch(mine, chunk):
        seq = row if mine else 1 - row
        src = own(chunk) if mine else None

        @pl.when(home)
        def _():
            if not mine:
                y_arrival(chunk).wait_recv()

            @pl.when(me < count - 1)
            def _():
                z_copy(0, seq, chunk, me, src).start()

            @pl.when(me > 0)
            def _():
                z_copy(1, seq, chunk, me, src).start()

    def spread(mine, chunk):
        seq = row if mine else 1 - row

        def turn(step, carry):
            for way in (0, 1):
                block = me - step if way == 0 else me + step
                inside = jnp.logical_and(
                    block >= row * half_blocks, block < (row + 1) * half_blocks
                )

                @pl.when(inside)
                def _():
                    z_copy(way, seq, chunk, block).wait_recv()

                    @pl.when(me < count - 1 if way == 0 else me > 0)
                    def _():
                        z_copy(way, seq, chunk, block).start()

            return carry

        lax.fori_loop(1, count, turn, 0)

    def own_place():
        return xs.at[
            row, :, pl.ds(pl.multiple_of((me - row * half_blocks) * width, width), width)
        ]

    def gain_columns(block):
        return gains_ref.at[:, pl.ds(pl.multiple_of(block * width, width), width)]

    def gain_copy(offset):
        return pltpu.make_async_remote_copy(
            src_ref=gain_tile,
            dst_ref=gain_columns(me),
            send_sem=g_send.at[offset],
            recv_sem=g_recv.at[me],
            device_id={"ma": (me + offset) % count},
            device_id_type=MESH,
        )

    def gain_arrival(block):
        return pltpu.make_async_remote_copy(
            src_ref=gain_tile,
            dst_ref=gain_columns(block),
            send_sem=g_send.at[0],
            recv_sem=g_recv.at[block],
            device_id={"ma": (me + 1) % count},
            device_id_type=MESH,
        )

    def wo_region(owner, piece, side):
        start = pl.multiple_of(owner * lane_rows + piece * piece_rows, piece_rows)
        return out_full_ref.at[
            pl.ds(start, piece_rows), pl.ds(pl.multiple_of(side * col_half, col_half), col_half)
        ]

    def wo_y(piece):
        start = pl.multiple_of(lane * lane_rows + piece * piece_rows, piece_rows)
        return pltpu.make_async_remote_copy(
            src_ref=wo_ref.at[pl.ds(start, piece_rows), :],
            dst_ref=wo_region(lane, piece, row),
            send_sem=wy_send.at[piece],
            recv_sem=wy_recv.at[piece],
            device_id={"row": 1 - row},
            device_id_type=MESH,
        )

    def wo_y_arrival(piece):
        here = wo_region(lane, piece, 1 - row)
        return pltpu.make_async_remote_copy(
            src_ref=here,
            dst_ref=here,
            send_sem=wy_send.at[piece],
            recv_sem=wy_recv.at[piece],
            device_id={"row": 1 - row},
            device_id_type=MESH,
        )

    def wo_fan(flip, piece, owner):
        here = wo_region(owner, piece, 1 - row)
        return pltpu.make_async_remote_copy(
            src_ref=here,
            dst_ref=here,
            send_sem=wf_send.at[flip - 1, piece],
            recv_sem=wf_recv.at[flip - 1, piece],
            device_id={"ba": ba ^ flip},
            device_id_type=MESH,
        )

    def part_copy(chunk, group):
        return pltpu.make_async_remote_copy(
            src_ref=part_out.at[chunk, group],
            dst_ref=part_in.at[chunk, group],
            send_sem=p_send.at[chunk, group],
            recv_sem=p_recv.at[chunk, group],
            device_id={"row": 1 - row},
            device_id_type=MESH,
        )

    def sum_copy(chunk):
        return pltpu.make_async_remote_copy(
            src_ref=sums_out.at[chunk],
            dst_ref=sums_in.at[chunk],
            send_sem=s_send.at[chunk],
            recv_sem=s_recv.at[chunk],
            device_id={"row": 1 - row},
            device_id_type=MESH,
        )

    launch(True, 0)

    @pl.when(jnp.logical_not(home))
    def _():
        for chunk in range(chunks):
            y_copy(chunk).start()

    for piece in range(pieces):
        wo_y(piece).start()

    half_lines = lax.broadcasted_iota(jnp.int32, gain_tile.shape, 0) < 8
    gain_tile[...] = jnp.where(
        half_lines,
        gain_ref[0:1, :].astype(jnp.float32),
        gain_ref[1:2, :].astype(jnp.float32),
    ).astype(jnp.bfloat16)

    def gain_send(offset, carry):
        gain_copy(offset).start()
        return carry

    lax.fori_loop(1, count, gain_send, 0)
    gain_local = pltpu.make_async_copy(gain_tile, gain_columns(me), gain_sem)
    gain_local.start()
    own_local = pltpu.make_async_copy(tok_ref, own_place(), own_sem)

    @pl.when(home)
    def _():
        own_local.start()

    wo_local = pltpu.make_async_copy(
        wo_ref,
        out_full_ref.at[:, pl.ds(pl.multiple_of(row * col_half, col_half), col_half)],
        wo_sem,
    )
    loads = [
        pltpu.make_async_copy(matrix, weights.at[index], w_sem.at[index])
        for index, matrix in enumerate((wq_ref, wk_ref, wv_ref))
    ]
    for load in loads:
        load.start()
    wo_local.start()

    span = 2 * length
    offset = lax.broadcasted_iota(jnp.int32, (8, span), 1) - (length - 1)
    distance = jnp.abs(offset)
    backward = jnp.zeros_like(distance)
    for threshold in bucket_thresholds[:15]:
        backward = backward + (distance >= threshold).astype(jnp.int32)
    forward = jnp.full_like(distance, 15)
    for threshold in bucket_thresholds:
        forward = forward + (distance >= threshold).astype(jnp.int32)
    bucket = jnp.where(offset > 0, forward, backward)

    def build_bias(head, carry):
        line = jnp.zeros((8, span), jnp.float32)
        for entry in range(table_ref.shape[0]):
            line = jnp.where(bucket == entry, table_ref[entry, head], line)
        tile = jnp.broadcast_to(line[0:1, :], (length, span))
        tile = pltpu.roll(tile, length + 1, 1, stride=1, stride_axis=0)
        bias[head] = tile[:, :length]
        return carry

    lax.fori_loop(0, heads, build_bias, 0)
    gain_local.wait()

    @pl.when(home)
    def _():
        own_local.wait()

    def gain_wait(step, carry):
        gain_arrival((me + step) % count).wait_recv()
        return carry

    lax.fori_loop(1, count, gain_wait, 0)
    gain_half = gains_ref[
        pl.ds(0, 8), pl.ds(pl.multiple_of(row * half, half), half)
    ][0:1, :].astype(jnp.float32)

    def multiply_gain(seq, start, size):
        values = xs[seq, pl.ds(start, size), :].astype(jnp.float32)
        scaled[pl.ds(start, size), :] = (values * gain_half).astype(jnp.bfloat16)
        return jnp.sum(values * values, axis=1, keepdims=True)

    def outgoing(chunk):
        squares = multiply_gain(1 - row, chunk * rows, rows)
        sums_out[chunk] = jnp.broadcast_to(squares, (rows, 128))
        sum_copy(chunk).start()

        def turn(group, carry):
            columns = pl.ds(pl.multiple_of(group * group_width, group_width), group_width)
            for index in range(3):
                part_out[chunk, group, :, pl.ds(index * group_width, group_width)] = jnp.dot(
                    scaled[pl.ds(chunk * rows, rows), :],
                    weights[index, :, columns],
                    preferred_element_type=jnp.float32,
                ).astype(jnp.bfloat16)
            part_copy(chunk, group).start()
            return carry

        lax.fori_loop(0, groups, turn, 0)

    def fan(piece):
        wo_y_arrival(piece).wait_recv()
        for flip in (1, 2, 3):
            wo_fan(flip, piece, lane).start()

    spread(True, 0)
    launch(False, 0)
    fan(0)
    spread(False, 0)
    launch(False, 1)
    for load in loads:
        load.wait()
    fan(1)
    outgoing(0)
    spread(False, 1)
    launch(True, 1)
    fan(2)
    outgoing(1)
    fan(3)
    spread(True, 1)
    own_squares = multiply_gain(row, 0, length)
    for chunk in range(chunks):
        sum_copy(chunk).wait_recv()
    other_squares = sums_in[...].reshape(length, 128)[:, 0:1]
    scale = lax.rsqrt((own_squares + other_squares) / (count * width) + epsilon)
    pair = 128 // head_size
    first_lanes = lax.broadcasted_iota(jnp.int32, (length, 128), 1)

    def attend(group, carry):
        columns = pl.ds(pl.multiple_of(group * group_width, group_width), group_width)
        products = [
            jnp.dot(scaled[...], weights[index, :, columns], preferred_element_type=jnp.float32)
            for index in range(3)
        ]
        for chunk in range(chunks):
            part_copy(chunk, group).wait_recv()
        query, key, value = [
            (
                (
                    product
                    + part_in[:, group, :, pl.ds(index * group_width, group_width)]
                    .astype(jnp.float32)
                    .reshape(length, group_width)
                )
                * scale
            ).astype(jnp.bfloat16)
            for index, product in enumerate(products)
        ]
        for tile in range(group_width // 128):
            cut = slice(tile * 128, (tile + 1) * 128)
            query_pair, key_pair, value_pair = query[:, cut], key[:, cut], value[:, cut]
            outcome = None
            for member in range(pair):
                mask = jnp.logical_and(
                    first_lanes >= member * head_size, first_lanes < (member + 1) * head_size
                )
                scores = (
                    lax.dot_general(
                        jnp.where(mask, query_pair.astype(jnp.float32), 0.0).astype(jnp.bfloat16),
                        key_pair,
                        (((1,), (1,)), ((), ())),
                        preferred_element_type=jnp.float32,
                    )
                    + bias[group * (group_width // head_size) + tile * pair + member]
                )
                exponent = jnp.exp(scores - jnp.max(scores, axis=1, keepdims=True))
                total = jnp.sum(exponent, axis=1, keepdims=True)
                mixed = jnp.dot(
                    (exponent / total).astype(jnp.bfloat16),
                    value_pair,
                    preferred_element_type=jnp.float32,
                )
                outcome = mixed if outcome is None else jnp.where(mask, mixed, outcome)
            att_ref[
                :, pl.ds(pl.multiple_of(group * group_width + tile * 128, 128), 128)
            ] = outcome.astype(jnp.bfloat16)
        return carry

    lax.fori_loop(0, groups, attend, 0)

    wo_local.wait()
    for piece in range(pieces):
        for flip in (1, 2, 3):
            wo_fan(flip, piece, lane ^ flip).wait_recv()
    for piece in range(pieces):
        wo_y(piece).wait_send()
        for flip in (1, 2, 3):
            wo_fan(flip, piece, lane).wait_send()
    for chunk in range(chunks):
        sum_copy(chunk).wait_send()

        def part_drain(group, carry):
            part_copy(chunk, group).wait_send()
            return carry

        lax.fori_loop(0, groups, part_drain, 0)

        @pl.when(jnp.logical_not(home))
        def _():
            y_copy(chunk).wait_send()

        def z_drain(slot, carry):
            block = slot + row * half_blocks
            for seq in (0, 1):

                @pl.when(jnp.logical_and(me < count - 1, block <= me))
                def _():
                    z_copy(0, seq, chunk, block).wait_send()

                @pl.when(jnp.logical_and(me > 0, block >= me))
                def _():
                    z_copy(1, seq, chunk, block).wait_send()

            return carry

        lax.fori_loop(0, half_blocks, z_drain, 0)

    def gain_drain(offset, carry):
        gain_copy(offset).wait_send()
        return carry

    lax.fori_loop(1, count, gain_drain, 0)


def front(tok, gains, table, wq, wk, wv, wo, count, collective_id):
    length, width = tok.shape
    chunks, pieces = 2, 4
    inner = wq.shape[1]
    heads = table.shape[1]
    head_size = inner // heads
    groups = max(1, inner // 256)
    half = wq.shape[0]
    rows = length // chunks
    group_width = inner // groups
    dma = pltpu.SemaphoreType.DMA
    vmem = pl.BlockSpec(memory_space=pltpu.VMEM)
    anywhere = pl.BlockSpec(memory_space=pl.ANY)
    parts = pltpu.VMEM((chunks, groups, rows, 3 * group_width), jnp.bfloat16)
    sums = pltpu.VMEM((chunks, rows, 128), jnp.float32)
    return pl.pallas_call(
        functools.partial(front_kernel, count, chunks, groups),
        out_shape=(
            jax.ShapeDtypeStruct((length, inner), jnp.bfloat16),
            jax.ShapeDtypeStruct((16, count * width), jnp.bfloat16),
            jax.ShapeDtypeStruct((wo.shape[0], 2 * wo.shape[1]), jnp.bfloat16),
        ),
        in_specs=[vmem, vmem, pl.BlockSpec(memory_space=pltpu.SMEM)] + [anywhere] * 4,
        out_specs=(vmem, vmem, vmem),
        scratch_shapes=[
            pltpu.VMEM((2, length, half), jnp.bfloat16),
            pltpu.VMEM((3, half, inner), jnp.bfloat16),
            pltpu.VMEM((length, half), jnp.bfloat16),
            parts,
            parts,
            sums,
            sums,
            pltpu.VMEM((heads, length, length), jnp.float32),
            pltpu.VMEM((16, width), jnp.bfloat16),
            dma((3,)),
            dma,
            dma,
            dma,
            dma((count,)),
            dma((count,)),
            dma((chunks,)),
            dma((chunks,)),
            dma((2, 2, chunks, count // 2)),
            dma((2, chunks, count // 2)),
            dma((chunks, groups)),
            dma((chunks, groups)),
            dma((chunks,)),
            dma((chunks,)),
            dma((pieces,)),
            dma((pieces,)),
            dma((3, pieces)),
            dma((3, pieces)),
        ],
        compiler_params=pltpu.CompilerParams(
            collective_id=collective_id, has_side_effects=True, vmem_limit_bytes=56 * 2**20
        ),
    )(tok, gains, table, wq, wk, wv, wo)


def on_device(
    tokens,
    attn_gain,
    query_weight,
    key_weight,
    value_projection_matrix,
    attention_output_matrix,
    bucket_bias_matrix,
    ffn_gain,
    gate_weight,
    up_weight,
    down_projection_weight,
):
    sequences, length, part_width = tokens.shape
    ma_count = lax.axis_size("ma")
    slab_rows = sequences * length
    token_rows = tokens.reshape(slab_rows, part_width)
    token_float = token_rows.astype(jnp.float32)
    attended, gains, out_full = front(
        token_rows,
        jnp.stack([attn_gain, ffn_gain]),
        bucket_bias_matrix,
        query_weight,
        key_weight,
        value_projection_matrix,
        attention_output_matrix,
        ma_count,
        3,
    )
    ffn_gain_full = gains[8]
    attn_out = reduce_all(attended, out_full, ma_count, 2, False, 2)
    residual_stream = (token_float + attn_out).astype(jnp.bfloat16)
    residual_f = residual_stream.astype(jnp.float32)
    gate_full, up_full, down_full = (gate_weight, up_weight, down_projection_weight)
    group_rows = gather_all(
        residual_stream, ma_count, (0, slab_rows // 2, slab_rows), False, 0
    )
    ffn_in = rms_scale(group_rows.astype(jnp.float32), ffn_gain_full)
    gate_act = jnp.dot(ffn_in, gate_full, preferred_element_type=jnp.float32)
    up_act = jnp.dot(ffn_in, up_full, preferred_element_type=jnp.float32)
    hidden = (jax.nn.gelu(gate_act, approximate=True) * up_act).astype(jnp.bfloat16)
    ffn_out = reduce_all(hidden, down_full, ma_count, 2, True, 1)
    encoded = (residual_f + ffn_out).astype(jnp.bfloat16)
    return encoded.reshape(sequences, length, part_width)


def solution(mesh):
    in_specs = (
        P(("ba", "row"), None, "ma"),
        P("ma"),
        P("row", "ma"),
        P("row", "ma"),
        P("row", "ma"),
        P("ma", "row"),
        P(None, "ma"),
        P("ma"),
        P(None, ("ma", "row")),
        P(None, ("ma", "row")),
        P(("ma", "row"), None),
    )
    out_specs = P(("ba", "row"), None, "ma")
    return jax.shard_map(
        on_device, mesh=mesh, in_specs=in_specs, out_specs=out_specs, check_vma=False
    )
```

```python
import functools

import jax
import jax.numpy as jnp
from jax import lax
from jax.experimental import pallas as pl
from jax.experimental.pallas import tpu as pltpu
from jax.sharding import PartitionSpec as P

bucket_thresholds = (1, 2, 3, 4, 5, 6, 7, 8, 11, 16, 23, 32, 45, 64, 91, 128)
epsilon = 1e-06


MESH = pl.DeviceIdType.MESH


def greet(me, count, row):
    barrier = pltpu.get_barrier_semaphore()

    @pl.when(me > 0)
    def _():
        pl.semaphore_signal(barrier, inc=1, device_id={"ma": me - 1}, device_id_type=MESH)

    @pl.when(me < count - 1)
    def _():
        pl.semaphore_signal(barrier, inc=1, device_id={"ma": me + 1}, device_id_type=MESH)

    pl.semaphore_signal(barrier, inc=1, device_id={"row": 1 - row}, device_id_type=MESH)
    inner = jnp.logical_and(me > 0, me < count - 1)
    pl.semaphore_wait(barrier, jnp.where(inner, 3, 2))


def front_kernel(
    count,
    chunks,
    groups,
    tok_ref,
    gain_ref,
    table_ref,
    wq_ref,
    wk_ref,
    wv_ref,
    wo_ref,
    share_ref,
    gains_ref,
    att_ref,
    out_full_ref,
    xs,
    weights,
    scaled,
    part_out,
    part_in,
    sums_out,
    sums_in,
    bias,
    gain_tile,
    w_sem,
    own_sem,
    gain_sem,
    wo_sem,
    g_send,
    g_recv,
    y_send,
    y_recv,
    z_send,
    z_recv,
    p_send,
    p_recv,
    s_send,
    s_recv,
    wy_send,
    wy_recv,
    wf_send,
    wf_recv,
):
    me = lax.axis_index("ma")
    row = lax.axis_index("row")
    ba = lax.axis_index("ba")
    length, width = tok_ref.shape
    half_blocks = count // 2
    half = half_blocks * width
    inner = att_ref.shape[1]
    heads = table_ref.shape[1]
    head_size = inner // heads
    rows = length // chunks
    group_width = inner // groups
    home = me // half_blocks == row
    col_half = wo_ref.shape[1]
    pieces = wy_send.shape[0]
    lane_rows = wo_ref.shape[0] // 4
    piece_rows = lane_rows // pieces
    lane = ba % 4

    barrier = pltpu.get_barrier_semaphore()

    def hello(offset, carry):
        pl.semaphore_signal(
            barrier, inc=1, device_id={"ma": (me + offset) % count}, device_id_type=MESH
        )
        return carry

    lax.fori_loop(1, count, hello, 0)
    pl.semaphore_signal(barrier, inc=1, device_id={"row": 1 - row}, device_id_type=MESH)
    for flip in (1, 2, 3):
        pl.semaphore_signal(barrier, inc=1, device_id={"ba": ba ^ flip}, device_id_type=MESH)
    pl.semaphore_wait(barrier, count + 3)

    def place(seq, chunk, slot):
        return xs.at[
            seq,
            pl.ds(chunk * rows, rows),
            pl.ds(pl.multiple_of(slot * width, width), width),
        ]

    def z_copy(way, seq, chunk, block, src=None):
        slot = block - row * half_blocks
        here = place(seq, chunk, slot)
        return pltpu.make_async_remote_copy(
            src_ref=here if src is None else src,
            dst_ref=here,
            send_sem=z_send.at[way, seq, chunk, slot],
            recv_sem=z_recv.at[seq, chunk, slot],
            device_id={"ma": me + 1 - 2 * way},
            device_id_type=MESH,
        )

    def own(chunk):
        return tok_ref.at[pl.ds(chunk * rows, rows), :]

    def y_copy(chunk):
        return pltpu.make_async_remote_copy(
            src_ref=own(chunk),
            dst_ref=place(row, chunk, me - (1 - row) * half_blocks),
            send_sem=y_send.at[chunk],
            recv_sem=y_recv.at[chunk],
            device_id={"row": 1 - row},
            device_id_type=MESH,
        )

    def y_arrival(chunk):
        here = place(1 - row, chunk, me - row * half_blocks)
        return pltpu.make_async_remote_copy(
            src_ref=here,
            dst_ref=here,
            send_sem=y_send.at[chunk],
            recv_sem=y_recv.at[chunk],
            device_id={"row": 1 - row},
            device_id_type=MESH,
        )

    def launch(mine, chunk):
        seq = row if mine else 1 - row
        src = own(chunk) if mine else None

        @pl.when(home)
        def _():
            if not mine:
                y_arrival(chunk).wait_recv()

            @pl.when(me < count - 1)
            def _():
                z_copy(0, seq, chunk, me, src).start()

            @pl.when(me > 0)
            def _():
                z_copy(1, seq, chunk, me, src).start()

    def spread(mine, chunk):
        seq = row if mine else 1 - row

        def turn(step, carry):
            for way in (0, 1):
                block = me - step if way == 0 else me + step
                inside = jnp.logical_and(
                    block >= row * half_blocks, block < (row + 1) * half_blocks
                )

                @pl.when(inside)
                def _():
                    z_copy(way, seq, chunk, block).wait_recv()

                    @pl.when(me < count - 1 if way == 0 else me > 0)
                    def _():
                        z_copy(way, seq, chunk, block).start()

            return carry

        lax.fori_loop(1, count, turn, 0)

    def own_place():
        return xs.at[
            row, :, pl.ds(pl.multiple_of((me - row * half_blocks) * width, width), width)
        ]

    def gain_columns(block):
        return gains_ref.at[:, pl.ds(pl.multiple_of(block * width, width), width)]

    def gain_copy(offset):
        return pltpu.make_async_remote_copy(
            src_ref=gain_tile,
            dst_ref=gain_columns(me),
            send_sem=g_send.at[offset],
            recv_sem=g_recv.at[me],
            device_id={"ma": (me + offset) % count},
            device_id_type=MESH,
        )

    def gain_arrival(block):
        return pltpu.make_async_remote_copy(
            src_ref=gain_tile,
            dst_ref=gain_columns(block),
            send_sem=g_send.at[0],
            recv_sem=g_recv.at[block],
            device_id={"ma": (me + 1) % count},
            device_id_type=MESH,
        )

    def wo_region(owner, piece, side):
        start = pl.multiple_of(owner * lane_rows + piece * piece_rows, piece_rows)
        return out_full_ref.at[
            pl.ds(start, piece_rows), pl.ds(pl.multiple_of(side * col_half, col_half), col_half)
        ]

    def wo_y(piece):
        start = pl.multiple_of(lane * lane_rows + piece * piece_rows, piece_rows)
        return pltpu.make_async_remote_copy(
            src_ref=wo_ref.at[pl.ds(start, piece_rows), :],
            dst_ref=wo_region(lane, piece, row),
            send_sem=wy_send.at[piece],
            recv_sem=wy_recv.at[piece],
            device_id={"row": 1 - row},
            device_id_type=MESH,
        )

    def wo_y_arrival(piece):
        here = wo_region(lane, piece, 1 - row)
        return pltpu.make_async_remote_copy(
            src_ref=here,
            dst_ref=here,
            send_sem=wy_send.at[piece],
            recv_sem=wy_recv.at[piece],
            device_id={"row": 1 - row},
            device_id_type=MESH,
        )

    def wo_fan(flip, piece, owner):
        here = wo_region(owner, piece, 1 - row)
        return pltpu.make_async_remote_copy(
            src_ref=here,
            dst_ref=here,
            send_sem=wf_send.at[flip - 1, piece],
            recv_sem=wf_recv.at[flip - 1, piece],
            device_id={"ba": ba ^ flip},
            device_id_type=MESH,
        )

    def part_copy(chunk, group):
        return pltpu.make_async_remote_copy(
            src_ref=part_out.at[chunk, group],
            dst_ref=part_in.at[chunk, group],
            send_sem=p_send.at[chunk, group],
            recv_sem=p_recv.at[chunk, group],
            device_id={"row": 1 - row},
            device_id_type=MESH,
        )

    def sum_copy(chunk):
        return pltpu.make_async_remote_copy(
            src_ref=sums_out.at[chunk],
            dst_ref=sums_in.at[chunk],
            send_sem=s_send.at[chunk],
            recv_sem=s_recv.at[chunk],
            device_id={"row": 1 - row},
            device_id_type=MESH,
        )

    launch(True, 0)

    @pl.when(jnp.logical_not(home))
    def _():
        for chunk in range(chunks):
            y_copy(chunk).start()

    for piece in range(pieces):
        wo_y(piece).start()

    half_lines = lax.broadcasted_iota(jnp.int32, gain_tile.shape, 0) < 8
    gain_tile[...] = jnp.where(
        half_lines,
        gain_ref[0:1, :].astype(jnp.float32),
        gain_ref[1:2, :].astype(jnp.float32),
    ).astype(jnp.bfloat16)

    def gain_send(offset, carry):
        gain_copy(offset).start()
        return carry

    lax.fori_loop(1, count, gain_send, 0)
    gain_local = pltpu.make_async_copy(gain_tile, gain_columns(me), gain_sem)
    gain_local.start()
    own_local = pltpu.make_async_copy(tok_ref, own_place(), own_sem)

    @pl.when(home)
    def _():
        own_local.start()

    wo_local = pltpu.make_async_copy(
        wo_ref,
        out_full_ref.at[:, pl.ds(pl.multiple_of(row * col_half, col_half), col_half)],
        wo_sem,
    )
    loads = [
        pltpu.make_async_copy(matrix, weights.at[index], w_sem.at[index])
        for index, matrix in enumerate((wq_ref, wk_ref, wv_ref))
    ]
    for load in loads:
        load.start()
    wo_local.start()

    span = 2 * length
    offset = lax.broadcasted_iota(jnp.int32, (8, span), 1) - (length - 1)
    distance = jnp.abs(offset)
    backward = jnp.zeros_like(distance)
    for threshold in bucket_thresholds[:15]:
        backward = backward + (distance >= threshold).astype(jnp.int32)
    forward = jnp.full_like(distance, 15)
    for threshold in bucket_thresholds:
        forward = forward + (distance >= threshold).astype(jnp.int32)
    bucket = jnp.where(offset > 0, forward, backward)

    def build_bias(head, carry):
        line = jnp.zeros((8, span), jnp.float32)
        for entry in range(table_ref.shape[0]):
            line = jnp.where(bucket == entry, table_ref[entry, head], line)
        tile = jnp.broadcast_to(line[0:1, :], (length, span))
        tile = pltpu.roll(tile, length + 1, 1, stride=1, stride_axis=0)
        bias[head] = tile[:, :length]
        return carry

    lax.fori_loop(0, heads, build_bias, 0)
    gain_local.wait()

    @pl.when(home)
    def _():
        own_local.wait()

    def gain_wait(step, carry):
        gain_arrival((me + step) % count).wait_recv()
        return carry

    lax.fori_loop(1, count, gain_wait, 0)
    gain_half = gains_ref[
        pl.ds(0, 8), pl.ds(pl.multiple_of(row * half, half), half)
    ][0:1, :].astype(jnp.float32)

    def multiply_gain(seq, start, size):
        values = xs[seq, pl.ds(start, size), :].astype(jnp.float32)
        scaled[pl.ds(start, size), :] = (values * gain_half).astype(jnp.bfloat16)
        return jnp.sum(values * values, axis=1, keepdims=True)

    def outgoing(chunk):
        squares = multiply_gain(1 - row, chunk * rows, rows)
        sums_out[chunk] = jnp.broadcast_to(squares, (rows, 128))
        sum_copy(chunk).start()

        def turn(group, carry):
            columns = pl.ds(pl.multiple_of(group * group_width, group_width), group_width)
            for index in range(3):
                part_out[chunk, group, :, pl.ds(index * group_width, group_width)] = jnp.dot(
                    scaled[pl.ds(chunk * rows, rows), :],
                    weights[index, :, columns],
                    preferred_element_type=jnp.float32,
                ).astype(jnp.bfloat16)
            part_copy(chunk, group).start()
            return carry

        lax.fori_loop(0, groups, turn, 0)

    def fan(piece):
        wo_y_arrival(piece).wait_recv()
        for flip in (1, 2, 3):
            wo_fan(flip, piece, lane).start()

    spread(True, 0)
    launch(False, 0)
    fan(0)
    spread(False, 0)
    launch(False, 1)
    for load in loads:
        load.wait()
    fan(1)
    outgoing(0)
    spread(False, 1)
    launch(True, 1)
    fan(2)
    outgoing(1)
    fan(3)
    spread(True, 1)
    own_squares = multiply_gain(row, 0, length)
    for chunk in range(chunks):
        sum_copy(chunk).wait_recv()
    other_squares = sums_in[...].reshape(length, 128)[:, 0:1]
    scale = lax.rsqrt((own_squares + other_squares) / (count * width) + epsilon)
    pair = 128 // head_size
    first_lanes = lax.broadcasted_iota(jnp.int32, (length, 128), 1)

    def attend(group, carry):
        columns = pl.ds(pl.multiple_of(group * group_width, group_width), group_width)
        products = [
            jnp.dot(scaled[...], weights[index, :, columns], preferred_element_type=jnp.float32)
            for index in range(3)
        ]
        for chunk in range(chunks):
            part_copy(chunk, group).wait_recv()
        query, key, value = [
            (
                (
                    product
                    + part_in[:, group, :, pl.ds(index * group_width, group_width)]
                    .astype(jnp.float32)
                    .reshape(length, group_width)
                )
                * scale
            ).astype(jnp.bfloat16)
            for index, product in enumerate(products)
        ]
        for tile in range(group_width // 128):
            cut = slice(tile * 128, (tile + 1) * 128)
            query_pair, key_pair, value_pair = query[:, cut], key[:, cut], value[:, cut]
            outcome = None
            for member in range(pair):
                mask = jnp.logical_and(
                    first_lanes >= member * head_size, first_lanes < (member + 1) * head_size
                )
                scores = (
                    lax.dot_general(
                        jnp.where(mask, query_pair.astype(jnp.float32), 0.0).astype(jnp.bfloat16),
                        key_pair,
                        (((1,), (1,)), ((), ())),
                        preferred_element_type=jnp.float32,
                    )
                    + bias[group * (group_width // head_size) + tile * pair + member]
                )
                exponent = jnp.exp(scores - jnp.max(scores, axis=1, keepdims=True))
                total = jnp.sum(exponent, axis=1, keepdims=True)
                mixed = jnp.dot(
                    (exponent / total).astype(jnp.bfloat16),
                    value_pair,
                    preferred_element_type=jnp.float32,
                )
                outcome = mixed if outcome is None else jnp.where(mask, mixed, outcome)
            att_ref[
                :, pl.ds(pl.multiple_of(group * group_width + tile * 128, 128), 128)
            ] = outcome.astype(jnp.bfloat16)
        return carry

    lax.fori_loop(0, groups, attend, 0)

    wo_local.wait()
    for piece in range(pieces):
        for flip in (1, 2, 3):
            wo_fan(flip, piece, lane ^ flip).wait_recv()

    def project(block, carry):
        columns = pl.ds(pl.multiple_of(block * width, width), width)
        share_ref[block] = jnp.dot(
            att_ref[...], out_full_ref[:, columns], preferred_element_type=jnp.float32
        ).astype(jnp.bfloat16)
        return carry

    lax.fori_loop(0, count, project, 0)
    for piece in range(pieces):
        wo_y(piece).wait_send()
        for flip in (1, 2, 3):
            wo_fan(flip, piece, lane).wait_send()
    for chunk in range(chunks):
        sum_copy(chunk).wait_send()

        def part_drain(group, carry):
            part_copy(chunk, group).wait_send()
            return carry

        lax.fori_loop(0, groups, part_drain, 0)

        @pl.when(jnp.logical_not(home))
        def _():
            y_copy(chunk).wait_send()

        def z_drain(slot, carry):
            block = slot + row * half_blocks
            for seq in (0, 1):

                @pl.when(jnp.logical_and(me < count - 1, block <= me))
                def _():
                    z_copy(0, seq, chunk, block).wait_send()

                @pl.when(jnp.logical_and(me > 0, block >= me))
                def _():
                    z_copy(1, seq, chunk, block).wait_send()

            return carry

        lax.fori_loop(0, half_blocks, z_drain, 0)

    def gain_drain(offset, carry):
        gain_copy(offset).wait_send()
        return carry

    lax.fori_loop(1, count, gain_drain, 0)


def front(tok, gains, table, wq, wk, wv, wo, count, collective_id):
    length, width = tok.shape
    chunks, pieces = 2, 4
    inner = wq.shape[1]
    heads = table.shape[1]
    head_size = inner // heads
    groups = max(1, inner // 256)
    half = wq.shape[0]
    rows = length // chunks
    group_width = inner // groups
    dma = pltpu.SemaphoreType.DMA
    vmem = pl.BlockSpec(memory_space=pltpu.VMEM)
    anywhere = pl.BlockSpec(memory_space=pl.ANY)
    parts = pltpu.VMEM((chunks, groups, rows, 3 * group_width), jnp.bfloat16)
    sums = pltpu.VMEM((chunks, rows, 128), jnp.float32)
    return pl.pallas_call(
        functools.partial(front_kernel, count, chunks, groups),
        out_shape=(
            jax.ShapeDtypeStruct((count, length, width), jnp.bfloat16),
            jax.ShapeDtypeStruct((16, count * width), jnp.bfloat16),
        ),
        in_specs=[vmem, vmem, pl.BlockSpec(memory_space=pltpu.SMEM)] + [anywhere] * 4,
        out_specs=(vmem, vmem),
        scratch_shapes=[
            pltpu.VMEM((length, inner), jnp.bfloat16),
            pltpu.VMEM((wo.shape[0], 2 * wo.shape[1]), jnp.bfloat16),
            pltpu.VMEM((2, length, half), jnp.bfloat16),
            pltpu.VMEM((3, half, inner), jnp.bfloat16),
            pltpu.VMEM((length, half), jnp.bfloat16),
            parts,
            parts,
            sums,
            sums,
            pltpu.VMEM((heads, length, length), jnp.float32),
            pltpu.VMEM((16, width), jnp.bfloat16),
            dma((3,)),
            dma,
            dma,
            dma,
            dma((count,)),
            dma((count,)),
            dma((chunks,)),
            dma((chunks,)),
            dma((2, 2, chunks, count // 2)),
            dma((2, chunks, count // 2)),
            dma((chunks, groups)),
            dma((chunks, groups)),
            dma((chunks,)),
            dma((chunks,)),
            dma((pieces,)),
            dma((pieces,)),
            dma((3, pieces)),
            dma((3, pieces)),
        ],
        compiler_params=pltpu.CompilerParams(
            collective_id=collective_id, has_side_effects=True, vmem_limit_bytes=56 * 2**20
        ),
    )(tok, gains, table, wq, wk, wv, wo)


def back_kernel(
    count,
    chunks,
    share_ref,
    gains_ref,
    tok_ref,
    gate_ref,
    up_ref,
    down_ref,
    out_ref,
    gate,
    up,
    down,
    group,
    normed,
    hidden,
    pair,
    kept,
    total,
    c_out,
    c_in,
    e_out,
    e_in,
    y_out,
    y_in,
    w_sem,
    c_send,
    c_recv,
    e_send,
    e_recv,
    y_send,
    y_recv,
    z_send,
    z_recv,
    x_send,
    x_recv,
):
    me = lax.axis_index("ma")
    row = lax.axis_index("row")
    length, width = tok_ref.shape
    rows = length // chunks
    greet(me, count, row)

    loads = [
        pltpu.make_async_copy(source, target, w_sem.at[index])
        for index, (source, target) in enumerate(
            ((gate_ref, gate), (up_ref, up), (down_ref, down))
        )
    ]
    for load in loads:
        load.start()

    def columns(block):
        return pl.ds(pl.multiple_of(block * width, width), width)

    def chunk_rows(chunk):
        return pl.ds(pl.multiple_of(chunk * rows, rows), rows)

    def hop(outs, ins, sends, recvs, chunk, block, rightward):
        slot = block if rightward else jnp.where(block == me - 1, count, block)
        return pltpu.make_async_remote_copy(
            src_ref=outs.at[chunk, block],
            dst_ref=ins.at[chunk, slot],
            send_sem=sends.at[chunk, block],
            recv_sem=recvs.at[chunk, slot],
            device_id={"ma": me + 1 if rightward else me - 1},
            device_id_type=MESH,
        )

    def landed(outs, ins, sends, recvs, chunk, slot, from_left):
        return pltpu.make_async_remote_copy(
            src_ref=outs.at[chunk, 0],
            dst_ref=ins.at[chunk, slot],
            send_sem=sends.at[chunk, 0],
            recv_sem=recvs.at[chunk, slot],
            device_id={"ma": me - 1 if from_left else me + 1},
            device_id_type=MESH,
        )

    def across(chunk, block):
        return pltpu.make_async_remote_copy(
            src_ref=y_out.at[chunk, block],
            dst_ref=y_in.at[chunk, block],
            send_sem=y_send.at[chunk, block],
            recv_sem=y_recv.at[chunk, block],
            device_id={"row": 1 - row},
            device_id_type=MESH,
        )

    def spot(chunk, seq, block):
        return group.at[chunk, seq, :, columns(block)]

    def pass_on(way, chunk, block):
        here = spot(chunk, row, block)
        return pltpu.make_async_remote_copy(
            src_ref=here,
            dst_ref=here,
            send_sem=z_send.at[way, chunk, block],
            recv_sem=z_recv.at[chunk, block],
            device_id={"ma": me + 1 - 2 * way},
            device_id_type=MESH,
        )

    def cross(chunk, seq, block):
        here = spot(chunk, seq, block)
        return pltpu.make_async_remote_copy(
            src_ref=here,
            dst_ref=here,
            send_sem=x_send.at[chunk, block],
            recv_sem=x_recv.at[chunk, block],
            device_id={"row": 1 - row},
            device_id_type=MESH,
        )

    def residual(chunk):
        group[chunk, row, :, columns(me)] = (
            tok_ref[chunk_rows(chunk), :].astype(jnp.float32) + total[...]
        ).astype(jnp.bfloat16)
        cross(chunk, row, me).start()

        @pl.when(me < count - 1)
        def _():
            pass_on(0, chunk, me).start()

        @pl.when(me > 0)
        def _():
            pass_on(1, chunk, me).start()

    def encode(chunk):
        out_ref[chunk_rows(chunk), :] = (
            group[chunk, row, :, columns(me)].astype(jnp.float32) + total[...]
        ).astype(jnp.bfloat16)

    attention_line = (c_out, c_in, c_send, c_recv)
    hidden_line = (e_out, e_in, e_send, e_recv)

    def chain(line, chunk, step, last):
        outs, ins, sends, recvs = line
        for rightward in (True, False):
            block = me + step if rightward else me - step
            inside = jnp.logical_and(block >= 0, block < count)
            if not rightward:
                inside = jnp.logical_and(inside, step > 0)

            @pl.when(inside)
            def _():
                if last:
                    across(chunk, block).wait_recv()
                    total[...] = kept[chunk, block] + y_in[chunk, block].astype(jnp.float32)
                else:
                    total[...] = share_ref[block, chunk_rows(chunk), :].astype(jnp.float32)

                if rightward:

                    @pl.when(me > 0)
                    def _():
                        landed(*line, chunk, block, True).wait_recv()
                        total[...] = total[...] + ins[chunk, block].astype(jnp.float32)

                    @pl.when(jnp.logical_and(step == 0, me < count - 1))
                    def _():
                        landed(*line, chunk, count, False).wait_recv()
                        total[...] = total[...] + ins[chunk, count].astype(jnp.float32)

                    @pl.when(step == 0)
                    def _():
                        if last:
                            encode(chunk)
                        else:
                            residual(chunk)

                    @pl.when(step > 0)
                    def _():
                        outs[chunk, block] = total[...].astype(jnp.bfloat16)
                        hop(*line, chunk, block, True).start()

                else:

                    @pl.when(me < count - 1)
                    def _():
                        landed(*line, chunk, block, False).wait_recv()
                        total[...] = total[...] + ins[chunk, block].astype(jnp.float32)

                    outs[chunk, block] = total[...].astype(jnp.bfloat16)
                    hop(*line, chunk, block, False).start()

    def spread(chunk, step):
        for way in (0, 1):
            block = me - step if way == 0 else me + step

            @pl.when(jnp.logical_and(block >= 0, block < count))
            def _():
                pass_on(way, chunk, block).wait_recv()
                cross(chunk, row, block).start()

                @pl.when(me < count - 1 if way == 0 else me > 0)
                def _():
                    pass_on(way, chunk, block).start()

    tile = min(256, hidden.shape[1])
    norm_rows = 16

    def feed(chunk):
        def arrive(block, carry):
            cross(chunk, 1 - row, block).wait_recv()
            return carry

        lax.fori_loop(0, count, arrive, 0)
        for seq in (0, 1):

            def normalize(index, carry):
                start = pl.multiple_of(index * norm_rows, norm_rows)
                values = group[chunk, seq, pl.ds(start, norm_rows), :].astype(jnp.float32)
                mean_square = jnp.mean(values * values, axis=1, keepdims=True)
                normed[pl.ds(seq * rows + start, norm_rows), :] = (
                    values
                    * lax.rsqrt(mean_square + epsilon)
                    * gains_ref[8:9, :].astype(jnp.float32)
                ).astype(jnp.bfloat16)
                return carry

            lax.fori_loop(0, rows // norm_rows, normalize, 0)

        @pl.when(chunk == 0)
        def _():
            for load in loads:
                load.wait()

        def gated(index, carry):
            cut = pl.ds(pl.multiple_of(index * tile, tile), tile)
            gate_act = jnp.dot(normed[...], gate[:, cut], preferred_element_type=jnp.float32)
            up_act = jnp.dot(normed[...], up[:, cut], preferred_element_type=jnp.float32)
            hidden[:, cut] = (jax.nn.gelu(gate_act, approximate=True) * up_act).astype(
                jnp.bfloat16
            )
            return carry

        lax.fori_loop(0, hidden.shape[1] // tile, gated, 0)

        def contract(index, carry):
            step = count - 1 - index // 2
            rightward = index % 2 == 0
            block = jnp.where(rightward, me + step, me - step)
            inside = jnp.logical_and(block >= 0, block < count)

            @pl.when(jnp.logical_and(inside, jnp.logical_or(step > 0, rightward)))
            def _():
                pair[...] = jnp.dot(
                    hidden[...], down[:, columns(block)], preferred_element_type=jnp.float32
                ).reshape(2, rows, width)
                y_out[chunk, block] = pair[1 - row].astype(jnp.bfloat16)
                across(chunk, block).start()
                kept[chunk, block] = pair[row]

            return carry

        lax.fori_loop(0, 2 * count, contract, 0)

    def tick(time, carry):
        shifted = time + 4 * count
        for line, base, last in (
            (attention_line, 0, False),
            (None, count - 1, False),
            (hidden_line, 2 * count + 1, True),
        ):
            for index in reversed(range(count // 2)):
                hop_index = 2 * index + (shifted - base) % 2
                chunk = (shifted - base - hop_index) // 2 - 2 * count
                active = jnp.logical_and(chunk >= 0, chunk < chunks)
                if line is None:

                    @pl.when(jnp.logical_and(active, hop_index > 0))
                    def _():
                        spread(chunk, hop_index)

                else:

                    @pl.when(active)
                    def _():
                        chain(line, chunk, count - 1 - hop_index, last)

        chunk = shifted // 2 - 3 * count

        @pl.when(
            jnp.logical_and(time % 2 == 0, jnp.logical_and(chunk >= 0, chunk < chunks))
        )
        def _():
            feed(chunk)

        return carry

    lax.fori_loop(0, 2 * chunks + 3 * count - 1, tick, 0)

    def drain(index, carry):
        chunk = index // count
        block = index % count
        across(chunk, block).wait_send()
        cross(chunk, row, block).wait_send()

        @pl.when(block > me)
        def _():
            hop(*attention_line, chunk, block, True).wait_send()
            hop(*hidden_line, chunk, block, True).wait_send()

        @pl.when(block < me)
        def _():
            hop(*attention_line, chunk, block, False).wait_send()
            hop(*hidden_line, chunk, block, False).wait_send()

        @pl.when(jnp.logical_and(me < count - 1, block <= me))
        def _():
            pass_on(0, chunk, block).wait_send()

        @pl.when(jnp.logical_and(me > 0, block >= me))
        def _():
            pass_on(1, chunk, block).wait_send()

        return carry

    lax.fori_loop(0, chunks * count, drain, 0)


def back(share, gains, tok, gate, up, down, count, chunks, collective_id):
    length, width = tok.shape
    rows = length // chunks
    inner = down.shape[0]
    dma = pltpu.SemaphoreType.DMA
    vmem = pl.BlockSpec(memory_space=pltpu.VMEM)
    anywhere = pl.BlockSpec(memory_space=pl.ANY)
    line = pltpu.VMEM((chunks, count, rows, width), jnp.bfloat16)
    longer = pltpu.VMEM((chunks, count + 1, rows, width), jnp.bfloat16)
    return pl.pallas_call(
        functools.partial(back_kernel, count, chunks),
        out_shape=jax.ShapeDtypeStruct((length, width), jnp.bfloat16),
        in_specs=[vmem, vmem, vmem] + [anywhere] * 3,
        out_specs=vmem,
        scratch_shapes=[
            pltpu.VMEM(gate.shape, jnp.bfloat16),
            pltpu.VMEM(up.shape, jnp.bfloat16),
            pltpu.VMEM(down.shape, jnp.bfloat16),
            pltpu.VMEM((chunks, 2, rows, count * width), jnp.bfloat16),
            pltpu.VMEM((2 * rows, count * width), jnp.bfloat16),
            pltpu.VMEM((2 * rows, inner), jnp.bfloat16),
            pltpu.VMEM((2, rows, width), jnp.float32),
            pltpu.VMEM((chunks, count, rows, width), jnp.float32),
            pltpu.VMEM((rows, width), jnp.float32),
            line,
            longer,
            line,
            longer,
            line,
            line,
            dma((3,)),
            dma((chunks, count)),
            dma((chunks, count + 1)),
            dma((chunks, count)),
            dma((chunks, count + 1)),
            dma((chunks, count)),
            dma((chunks, count)),
            dma((2, chunks, count)),
            dma((chunks, count)),
            dma((chunks, count)),
            dma((chunks, count)),
        ],
        compiler_params=pltpu.CompilerParams(
            collective_id=collective_id, has_side_effects=True, vmem_limit_bytes=60 * 2**20
        ),
    )(share, gains, tok, gate, up, down)


def on_device(
    tokens,
    attn_gain,
    query_weight,
    key_weight,
    value_projection_matrix,
    attention_output_matrix,
    bucket_bias_matrix,
    ffn_gain,
    gate_weight,
    up_weight,
    down_projection_weight,
):
    sequences, length, part_width = tokens.shape
    ma_count = lax.axis_size("ma")
    slab_rows = sequences * length
    token_rows = tokens.reshape(slab_rows, part_width)
    share, gains = front(
        token_rows,
        jnp.stack([attn_gain, ffn_gain]),
        bucket_bias_matrix,
        query_weight,
        key_weight,
        value_projection_matrix,
        attention_output_matrix,
        ma_count,
        3,
    )
    encoded = back(
        share,
        gains,
        token_rows,
        gate_weight,
        up_weight,
        down_projection_weight,
        ma_count,
        4,
        1,
    )
    return encoded.reshape(sequences, length, part_width)


def solution(mesh):
    in_specs = (
        P(("ba", "row"), None, "ma"),
        P("ma"),
        P("row", "ma"),
        P("row", "ma"),
        P("row", "ma"),
        P("ma", "row"),
        P(None, "ma"),
        P("ma"),
        P(None, ("ma", "row")),
        P(None, ("ma", "row")),
        P(("ma", "row"), None),
    )
    out_specs = P(("ba", "row"), None, "ma")
    return jax.shard_map(
        on_device, mesh=mesh, in_specs=in_specs, out_specs=out_specs, check_vma=False
    )
```

```python
import functools

import jax
import jax.numpy as jnp
from jax import lax
from jax.experimental import pallas as pl
from jax.experimental.pallas import tpu as pltpu
from jax.sharding import PartitionSpec as P

bucket_thresholds = (1, 2, 3, 4, 5, 6, 7, 8, 11, 16, 23, 32, 45, 64, 91, 128)
epsilon = 1e-06


MESH = pl.DeviceIdType.MESH


def greet(me, count, row):
    barrier = pltpu.get_barrier_semaphore()

    @pl.when(me > 0)
    def _():
        pl.semaphore_signal(barrier, inc=1, device_id={"ma": me - 1}, device_id_type=MESH)

    @pl.when(me < count - 1)
    def _():
        pl.semaphore_signal(barrier, inc=1, device_id={"ma": me + 1}, device_id_type=MESH)

    pl.semaphore_signal(barrier, inc=1, device_id={"row": 1 - row}, device_id_type=MESH)
    inner = jnp.logical_and(me > 0, me < count - 1)
    pl.semaphore_wait(barrier, jnp.where(inner, 3, 2))


def front_kernel(
    count,
    chunks,
    groups,
    tok_ref,
    attn_gain_ref,
    ffn_gain_ref,
    table_ref,
    wq_ref,
    wk_ref,
    wv_ref,
    wo_ref,
    share_ref,
    gains_ref,
    att_ref,
    out_full_ref,
    xs,
    weights,
    scaled,
    part_out,
    part_in,
    sums_out,
    sums_in,
    bias,
    lines,
    gain_tile,
    w_sem,
    own_sem,
    gain_sem,
    wo_sem,
    g_send,
    g_recv,
    y_send,
    y_recv,
    z_send,
    z_recv,
    p_send,
    p_recv,
    s_send,
    s_recv,
    wy_send,
    wy_recv,
    wf_send,
    wf_recv,
):
    me = lax.axis_index("ma")
    row = lax.axis_index("row")
    ba = lax.axis_index("ba")
    length, width = tok_ref.shape
    half_blocks = count // 2
    half = half_blocks * width
    inner = att_ref.shape[1]
    heads = table_ref.shape[1]
    head_size = inner // heads
    rows = length // chunks
    group_width = inner // groups
    home = me // half_blocks == row
    col_half = wo_ref.shape[1]
    pieces = wy_send.shape[0]
    lane_rows = wo_ref.shape[0] // 4
    piece_rows = lane_rows // pieces
    lane = ba % 4

    barrier = pltpu.get_barrier_semaphore()

    def hello(offset, carry):
        pl.semaphore_signal(
            barrier, inc=1, device_id={"ma": (me + offset) % count}, device_id_type=MESH
        )
        return carry

    lax.fori_loop(1, count, hello, 0)
    pl.semaphore_signal(barrier, inc=1, device_id={"row": 1 - row}, device_id_type=MESH)
    for flip in (1, 2, 3):
        pl.semaphore_signal(barrier, inc=1, device_id={"ba": ba ^ flip}, device_id_type=MESH)
    pl.semaphore_wait(barrier, count + 3)

    def place(seq, chunk, slot):
        return xs.at[
            seq,
            pl.ds(chunk * rows, rows),
            pl.ds(pl.multiple_of(slot * width, width), width),
        ]

    def z_copy(way, seq, chunk, block, src=None):
        slot = block - row * half_blocks
        here = place(seq, chunk, slot)
        return pltpu.make_async_remote_copy(
            src_ref=here if src is None else src,
            dst_ref=here,
            send_sem=z_send.at[way, seq, chunk, slot],
            recv_sem=z_recv.at[seq, chunk, slot],
            device_id={"ma": me + 1 - 2 * way},
            device_id_type=MESH,
        )

    def own(chunk):
        return tok_ref.at[pl.ds(chunk * rows, rows), :]

    def y_copy(chunk):
        return pltpu.make_async_remote_copy(
            src_ref=own(chunk),
            dst_ref=place(row, chunk, me - (1 - row) * half_blocks),
            send_sem=y_send.at[chunk],
            recv_sem=y_recv.at[chunk],
            device_id={"row": 1 - row},
            device_id_type=MESH,
        )

    def y_arrival(chunk):
        here = place(1 - row, chunk, me - row * half_blocks)
        return pltpu.make_async_remote_copy(
            src_ref=here,
            dst_ref=here,
            send_sem=y_send.at[chunk],
            recv_sem=y_recv.at[chunk],
            device_id={"row": 1 - row},
            device_id_type=MESH,
        )

    def launch(mine, chunk):
        seq = row if mine else 1 - row
        src = own(chunk) if mine else None

        @pl.when(home)
        def _():
            if not mine:
                y_arrival(chunk).wait_recv()

            @pl.when(me < count - 1)
            def _():
                z_copy(0, seq, chunk, me, src).start()

            @pl.when(me > 0)
            def _():
                z_copy(1, seq, chunk, me, src).start()

    def spread(mine, chunk):
        seq = row if mine else 1 - row

        def turn(step, carry):
            for way in (0, 1):
                block = me - step if way == 0 else me + step
                inside = jnp.logical_and(
                    block >= row * half_blocks, block < (row + 1) * half_blocks
                )

                @pl.when(inside)
                def _():
                    z_copy(way, seq, chunk, block).wait_recv()

                    @pl.when(me < count - 1 if way == 0 else me > 0)
                    def _():
                        z_copy(way, seq, chunk, block).start()

            return carry

        lax.fori_loop(1, count, turn, 0)

    def own_place():
        return xs.at[
            row, :, pl.ds(pl.multiple_of((me - row * half_blocks) * width, width), width)
        ]

    def gain_columns(block):
        return gains_ref.at[:, pl.ds(pl.multiple_of(block * width, width), width)]

    def gain_copy(offset):
        return pltpu.make_async_remote_copy(
            src_ref=gain_tile,
            dst_ref=gain_columns(me),
            send_sem=g_send.at[offset],
            recv_sem=g_recv.at[me],
            device_id={"ma": (me + offset) % count},
            device_id_type=MESH,
        )

    def gain_arrival(block):
        return pltpu.make_async_remote_copy(
            src_ref=gain_tile,
            dst_ref=gain_columns(block),
            send_sem=g_send.at[0],
            recv_sem=g_recv.at[block],
            device_id={"ma": (me + 1) % count},
            device_id_type=MESH,
        )

    def wo_region(owner, piece, side):
        start = pl.multiple_of(owner * lane_rows + piece * piece_rows, piece_rows)
        return out_full_ref.at[
            pl.ds(start, piece_rows), pl.ds(pl.multiple_of(side * col_half, col_half), col_half)
        ]

    def wo_y(piece):
        start = pl.multiple_of(lane * lane_rows + piece * piece_rows, piece_rows)
        return pltpu.make_async_remote_copy(
            src_ref=wo_ref.at[pl.ds(start, piece_rows), :],
            dst_ref=wo_region(lane, piece, row),
            send_sem=wy_send.at[piece],
            recv_sem=wy_recv.at[piece],
            device_id={"row": 1 - row},
            device_id_type=MESH,
        )

    def wo_y_arrival(piece):
        here = wo_region(lane, piece, 1 - row)
        return pltpu.make_async_remote_copy(
            src_ref=here,
            dst_ref=here,
            send_sem=wy_send.at[piece],
            recv_sem=wy_recv.at[piece],
            device_id={"row": 1 - row},
            device_id_type=MESH,
        )

    def wo_fan(flip, piece, owner):
        here = wo_region(owner, piece, 1 - row)
        return pltpu.make_async_remote_copy(
            src_ref=here,
            dst_ref=here,
            send_sem=wf_send.at[flip - 1, piece],
            recv_sem=wf_recv.at[flip - 1, piece],
            device_id={"ba": ba ^ flip},
            device_id_type=MESH,
        )

    def part_copy(chunk, group):
        return pltpu.make_async_remote_copy(
            src_ref=part_out.at[chunk, group],
            dst_ref=part_in.at[chunk, group],
            send_sem=p_send.at[chunk, group],
            recv_sem=p_recv.at[chunk, group],
            device_id={"row": 1 - row},
            device_id_type=MESH,
        )

    def sum_copy(chunk):
        return pltpu.make_async_remote_copy(
            src_ref=sums_out.at[chunk],
            dst_ref=sums_in.at[chunk],
            send_sem=s_send.at[chunk],
            recv_sem=s_recv.at[chunk],
            device_id={"row": 1 - row},
            device_id_type=MESH,
        )

    launch(True, 0)

    @pl.when(jnp.logical_not(home))
    def _():
        for chunk in range(chunks):
            y_copy(chunk).start()

    for piece in range(pieces):
        wo_y(piece).start()

    half_lines = lax.broadcasted_iota(jnp.int32, gain_tile.shape, 0) < 8
    gain_tile[...] = jnp.where(
        half_lines,
        jnp.broadcast_to(attn_gain_ref[...].astype(jnp.float32)[None, :], gain_tile.shape),
        jnp.broadcast_to(ffn_gain_ref[...].astype(jnp.float32)[None, :], gain_tile.shape),
    ).astype(jnp.bfloat16)

    def gain_send(offset, carry):
        gain_copy(offset).start()
        return carry

    lax.fori_loop(1, count, gain_send, 0)
    gain_local = pltpu.make_async_copy(gain_tile, gain_columns(me), gain_sem)
    gain_local.start()
    own_local = pltpu.make_async_copy(tok_ref, own_place(), own_sem)

    @pl.when(home)
    def _():
        own_local.start()

    wo_local = pltpu.make_async_copy(
        wo_ref,
        out_full_ref.at[:, pl.ds(pl.multiple_of(row * col_half, col_half), col_half)],
        wo_sem,
    )
    loads = [
        pltpu.make_async_copy(matrix, weights.at[index], w_sem.at[index])
        for index, matrix in enumerate((wq_ref, wk_ref, wv_ref))
    ]
    for load in loads:
        load.start()
    wo_local.start()

    span = 2 * length
    offset = lax.broadcasted_iota(jnp.int32, (8, span), 1) - (length - 1)
    distance = jnp.abs(offset)
    backward = jnp.zeros_like(distance)
    for threshold in bucket_thresholds[:15]:
        backward = backward + (distance >= threshold).astype(jnp.int32)
    forward = jnp.full_like(distance, 15)
    for threshold in bucket_thresholds:
        forward = forward + (distance >= threshold).astype(jnp.int32)
    bucket = jnp.where(offset > 0, forward, backward)

    entries = lax.broadcasted_iota(jnp.int32, (table_ref.shape[0], span), 0)
    chosen = (entries == jnp.broadcast_to(bucket[0:1, :], entries.shape)).astype(jnp.float32)
    lines[...] = lax.dot_general(
        table_ref[...],
        chosen,
        (((0,), (0,)), ((), ())),
        precision=lax.Precision.HIGHEST,
        preferred_element_type=jnp.float32,
    )

    def build_bias(head, carry):
        tile = jnp.broadcast_to(lines[pl.ds(head, 1), :], (length, span))
        tile = pltpu.roll(tile, length + 1, 1, stride=1, stride_axis=0)
        bias[head] = tile[:, :length]
        return carry

    lax.fori_loop(0, heads, build_bias, 0)
    gain_local.wait()

    @pl.when(home)
    def _():
        own_local.wait()

    def gain_wait(step, carry):
        gain_arrival((me + step) % count).wait_recv()
        return carry

    lax.fori_loop(1, count, gain_wait, 0)
    gain_half = gains_ref[
        pl.ds(0, 8), pl.ds(pl.multiple_of(row * half, half), half)
    ][0:1, :].astype(jnp.float32)

    def multiply_gain(seq, start, size):
        values = xs[seq, pl.ds(start, size), :].astype(jnp.float32)
        scaled[pl.ds(start, size), :] = (values * gain_half).astype(jnp.bfloat16)
        return jnp.sum(values * values, axis=1, keepdims=True)

    def outgoing(chunk):
        squares = multiply_gain(1 - row, chunk * rows, rows)
        for start in range(0, rows, 128):
            sums_out[chunk, :, start : start + 128] = jnp.broadcast_to(
                squares[start : start + 128], (128, 128)
            ).T[0:8]
        sum_copy(chunk).start()

        def turn(group, carry):
            columns = pl.ds(pl.multiple_of(group * group_width, group_width), group_width)
            for index in range(3):
                part_out[chunk, group, :, pl.ds(index * group_width, group_width)] = jnp.dot(
                    scaled[pl.ds(chunk * rows, rows), :],
                    weights[index, :, columns],
                    preferred_element_type=jnp.float32,
                ).astype(jnp.bfloat16)
            part_copy(chunk, group).start()
            return carry

        lax.fori_loop(0, groups, turn, 0)

    def fan(piece):
        wo_y_arrival(piece).wait_recv()
        for flip in (1, 2, 3):
            wo_fan(flip, piece, lane).start()

    spread(True, 0)
    launch(False, 0)
    fan(0)
    spread(False, 0)
    launch(False, 1)
    for load in loads:
        load.wait()
    fan(1)
    outgoing(0)
    spread(False, 1)
    launch(True, 1)
    fan(2)
    outgoing(1)
    fan(3)
    spread(True, 1)
    own_squares = multiply_gain(row, 0, length)
    for chunk in range(chunks):
        sum_copy(chunk).wait_recv()
    other_squares = jnp.concatenate(
        [
            jnp.broadcast_to(sums_in[chunk, 0:1, start : start + 128], (128, 128)).T[:, 0:1]
            for chunk in range(chunks)
            for start in range(0, rows, 128)
        ]
    )
    scale = lax.rsqrt((own_squares + other_squares) / (count * width) + epsilon)
    pair = 128 // head_size
    first_lanes = lax.broadcasted_iota(jnp.int32, (length, 128), 1)

    def attend(group, carry):
        columns = pl.ds(pl.multiple_of(group * group_width, group_width), group_width)
        products = [
            jnp.dot(scaled[...], weights[index, :, columns], preferred_element_type=jnp.float32)
            for index in range(3)
        ]
        for chunk in range(chunks):
            part_copy(chunk, group).wait_recv()
        query, key, value = [
            (
                (
                    product
                    + part_in[:, group, :, pl.ds(index * group_width, group_width)]
                    .astype(jnp.float32)
                    .reshape(length, group_width)
                )
                * scale
            ).astype(jnp.bfloat16)
            for index, product in enumerate(products)
        ]
        for tile in range(group_width // 128):
            cut = slice(tile * 128, (tile + 1) * 128)
            query_pair, key_pair, value_pair = query[:, cut], key[:, cut], value[:, cut]
            outcome = None
            for member in range(pair):
                mask = jnp.logical_and(
                    first_lanes >= member * head_size, first_lanes < (member + 1) * head_size
                )
                scores = (
                    lax.dot_general(
                        jnp.where(mask, query_pair.astype(jnp.float32), 0.0).astype(jnp.bfloat16),
                        key_pair,
                        (((1,), (1,)), ((), ())),
                        preferred_element_type=jnp.float32,
                    )
                    + bias[group * (group_width // head_size) + tile * pair + member]
                )
                exponent = jnp.exp(scores - jnp.max(scores, axis=1, keepdims=True))
                total = jnp.sum(exponent, axis=1, keepdims=True)
                mixed = jnp.dot(
                    (exponent / total).astype(jnp.bfloat16),
                    value_pair,
                    preferred_element_type=jnp.float32,
                )
                outcome = mixed if outcome is None else jnp.where(mask, mixed, outcome)
            att_ref[
                :, pl.ds(pl.multiple_of(group * group_width + tile * 128, 128), 128)
            ] = outcome.astype(jnp.bfloat16)
        return carry

    lax.fori_loop(0, groups, attend, 0)

    wo_local.wait()
    for piece in range(pieces):
        for flip in (1, 2, 3):
            wo_fan(flip, piece, lane ^ flip).wait_recv()

    def project(block, carry):
        columns = pl.ds(pl.multiple_of(block * width, width), width)
        share_ref[block] = jnp.dot(
            att_ref[...], out_full_ref[:, columns], preferred_element_type=jnp.float32
        ).astype(jnp.bfloat16)
        return carry

    lax.fori_loop(0, count, project, 0)
    for piece in range(pieces):
        wo_y(piece).wait_send()
        for flip in (1, 2, 3):
            wo_fan(flip, piece, lane).wait_send()
    for chunk in range(chunks):
        sum_copy(chunk).wait_send()

        def part_drain(group, carry):
            part_copy(chunk, group).wait_send()
            return carry

        lax.fori_loop(0, groups, part_drain, 0)

        @pl.when(jnp.logical_not(home))
        def _():
            y_copy(chunk).wait_send()

        def z_drain(slot, carry):
            block = slot + row * half_blocks
            for seq in (0, 1):

                @pl.when(jnp.logical_and(me < count - 1, block <= me))
                def _():
                    z_copy(0, seq, chunk, block).wait_send()

                @pl.when(jnp.logical_and(me > 0, block >= me))
                def _():
                    z_copy(1, seq, chunk, block).wait_send()

            return carry

        lax.fori_loop(0, half_blocks, z_drain, 0)

    def gain_drain(offset, carry):
        gain_copy(offset).wait_send()
        return carry

    lax.fori_loop(1, count, gain_drain, 0)


def front(tok, attn_gain, ffn_gain, table, wq, wk, wv, wo, count, collective_id):
    length, width = tok.shape
    chunks, pieces = 2, 4
    inner = wq.shape[1]
    heads = table.shape[1]
    head_size = inner // heads
    groups = max(1, inner // 256)
    half = wq.shape[0]
    rows = length // chunks
    group_width = inner // groups
    dma = pltpu.SemaphoreType.DMA
    vmem = pl.BlockSpec(memory_space=pltpu.VMEM)
    anywhere = pl.BlockSpec(memory_space=pl.ANY)
    parts = pltpu.VMEM((chunks, groups, rows, 3 * group_width), jnp.bfloat16)
    sums = pltpu.VMEM((chunks, 8, rows), jnp.float32)
    return pl.pallas_call(
        functools.partial(front_kernel, count, chunks, groups),
        out_shape=(
            jax.ShapeDtypeStruct((count, length, width), jnp.bfloat16),
            jax.ShapeDtypeStruct((16, count * width), jnp.bfloat16),
        ),
        in_specs=[vmem] * 4 + [anywhere] * 4,
        out_specs=(vmem, vmem),
        scratch_shapes=[
            pltpu.VMEM((length, inner), jnp.bfloat16),
            pltpu.VMEM((wo.shape[0], 2 * wo.shape[1]), jnp.bfloat16),
            pltpu.VMEM((2, length, half), jnp.bfloat16),
            pltpu.VMEM((3, half, inner), jnp.bfloat16),
            pltpu.VMEM((length, half), jnp.bfloat16),
            parts,
            parts,
            sums,
            sums,
            pltpu.VMEM((heads, length, length), jnp.float32),
            pltpu.VMEM((heads, 2 * length), jnp.float32),
            pltpu.VMEM((16, width), jnp.bfloat16),
            dma((3,)),
            dma,
            dma,
            dma,
            dma((count,)),
            dma((count,)),
            dma((chunks,)),
            dma((chunks,)),
            dma((2, 2, chunks, count // 2)),
            dma((2, chunks, count // 2)),
            dma((chunks, groups)),
            dma((chunks, groups)),
            dma((chunks,)),
            dma((chunks,)),
            dma((pieces,)),
            dma((pieces,)),
            dma((3, pieces)),
            dma((3, pieces)),
        ],
        compiler_params=pltpu.CompilerParams(
            collective_id=collective_id, has_side_effects=True, vmem_limit_bytes=56 * 2**20
        ),
    )(tok, attn_gain, ffn_gain, table, wq, wk, wv, wo)


def back_kernel(
    count,
    chunks,
    per,
    spacing,
    share_ref,
    gains_ref,
    tok_ref,
    gate_ref,
    up_ref,
    down_ref,
    out_ref,
    gate,
    up,
    down,
    group,
    normed,
    hidden,
    pair,
    kept,
    total,
    c_out,
    c_in,
    e_out,
    e_in,
    y_out,
    y_in,
    w_sem,
    c_send,
    c_recv,
    e_send,
    e_recv,
    y_send,
    y_recv,
    z_send,
    z_recv,
    x_send,
    x_recv,
    r_send,
    r_recv,
):
    me = lax.axis_index("ma")
    row = lax.axis_index("row")
    length, width = tok_ref.shape
    rows = length // chunks
    greet(me, count, row)

    loads = [
        pltpu.make_async_copy(source, target, w_sem.at[index])
        for index, (source, target) in enumerate(
            ((gate_ref, gate), (up_ref, up), (down_ref, down))
        )
    ]
    for load in loads:
        load.start()

    def columns(block):
        return pl.ds(pl.multiple_of(block * width, width), width)

    def chunk_rows(chunk):
        return pl.ds(pl.multiple_of(chunk * rows, rows), rows)

    def hop(outs, ins, sends, recvs, chunk, block, rightward):
        slot = block if rightward else jnp.where(block == me - 1, count, block)
        return pltpu.make_async_remote_copy(
            src_ref=outs.at[chunk, block],
            dst_ref=ins.at[chunk, slot],
            send_sem=sends.at[chunk, block],
            recv_sem=recvs.at[chunk, slot],
            device_id={"ma": me + 1 if rightward else me - 1},
            device_id_type=MESH,
        )

    def landed(outs, ins, sends, recvs, chunk, slot, from_left):
        return pltpu.make_async_remote_copy(
            src_ref=outs.at[chunk, 0],
            dst_ref=ins.at[chunk, slot],
            send_sem=sends.at[chunk, 0],
            recv_sem=recvs.at[chunk, slot],
            device_id={"ma": me - 1 if from_left else me + 1},
            device_id_type=MESH,
        )

    def across(chunk, block):
        return pltpu.make_async_remote_copy(
            src_ref=y_out.at[chunk, block],
            dst_ref=y_in.at[chunk, block],
            send_sem=y_send.at[chunk, block],
            recv_sem=y_recv.at[chunk, block],
            device_id={"row": 1 - row},
            device_id_type=MESH,
        )

    def spot(chunk, seq, block):
        return group.at[chunk, seq, :, columns(block)]

    def pass_on(way, chunk, block):
        here = spot(chunk, row, block)
        return pltpu.make_async_remote_copy(
            src_ref=here,
            dst_ref=here,
            send_sem=z_send.at[way, chunk, block],
            recv_sem=z_recv.at[chunk, block],
            device_id={"ma": me + 1 - 2 * way},
            device_id_type=MESH,
        )

    def cross(chunk, seq, block):
        here = spot(chunk, seq, block)
        return pltpu.make_async_remote_copy(
            src_ref=here,
            dst_ref=here,
            send_sem=x_send.at[chunk, block],
            recv_sem=x_recv.at[chunk, block],
            device_id={"row": 1 - row},
            device_id_type=MESH,
        )

    middle = count // 2

    def crosses(block):
        return jnp.logical_not(
            jnp.logical_or(
                jnp.logical_and(block == 0, me >= middle),
                jnp.logical_and(block == count - 1, me < middle),
            )
        )

    def relay(end, chunk):
        here = spot(chunk, 1 - row, end * (count - 1))
        return pltpu.make_async_remote_copy(
            src_ref=here,
            dst_ref=here,
            send_sem=r_send.at[end, chunk],
            recv_sem=r_recv.at[end, chunk],
            device_id={"ma": me + 1 - 2 * end},
            device_id_type=MESH,
        )

    def relay_turn(end):
        return me - (middle - 1) if end == 0 else middle - me

    def relays(end):
        turn = relay_turn(end)
        return jnp.logical_and(turn >= 0, turn < middle)

    def residual(chunk):
        group[chunk, row, :, columns(me)] = (
            tok_ref[chunk_rows(chunk), :].astype(jnp.float32) + total[...]
        ).astype(jnp.bfloat16)
        cross(chunk, row, me).start()

        @pl.when(me < count - 1)
        def _():
            pass_on(0, chunk, me).start()

        @pl.when(me > 0)
        def _():
            pass_on(1, chunk, me).start()

    def encode(chunk):
        out_ref[chunk_rows(chunk), :] = (
            group[chunk, row, :, columns(me)].astype(jnp.float32) + total[...]
        ).astype(jnp.bfloat16)

    attention_line = (c_out, c_in, c_send, c_recv)
    hidden_line = (e_out, e_in, e_send, e_recv)

    def chain(line, chunk, step, last):
        outs, ins, sends, recvs = line
        for rightward in (True, False):
            block = me + step if rightward else me - step
            inside = jnp.logical_and(block >= 0, block < count)
            if not rightward:
                inside = jnp.logical_and(inside, step > 0)

            @pl.when(inside)
            def _():
                if last:
                    across(chunk, block).wait_recv()
                    total[...] = kept[chunk, block] + y_in[chunk, block].astype(jnp.float32)
                else:
                    total[...] = share_ref[block, chunk_rows(chunk), :].astype(jnp.float32)

                if rightward:

                    @pl.when(me > 0)
                    def _():
                        landed(*line, chunk, block, True).wait_recv()
                        total[...] = total[...] + ins[chunk, block].astype(jnp.float32)

                    @pl.when(jnp.logical_and(step == 0, me < count - 1))
                    def _():
                        landed(*line, chunk, count, False).wait_recv()
                        total[...] = total[...] + ins[chunk, count].astype(jnp.float32)

                    @pl.when(step == 0)
                    def _():
                        if last:
                            encode(chunk)
                        else:
                            residual(chunk)

                    @pl.when(step > 0)
                    def _():
                        outs[chunk, block] = total[...].astype(jnp.bfloat16)
                        hop(*line, chunk, block, True).start()

                else:

                    @pl.when(me < count - 1)
                    def _():
                        landed(*line, chunk, block, False).wait_recv()
                        total[...] = total[...] + ins[chunk, block].astype(jnp.float32)

                    outs[chunk, block] = total[...].astype(jnp.bfloat16)
                    hop(*line, chunk, block, False).start()

    def spread(chunk, step):
        for way in (0, 1):
            block = me - step if way == 0 else me + step

            @pl.when(jnp.logical_and(block >= 0, block < count))
            def _():
                pass_on(way, chunk, block).wait_recv()

                @pl.when(crosses(block))
                def _():
                    cross(chunk, row, block).start()

                @pl.when(me < count - 1 if way == 0 else me > 0)
                def _():
                    pass_on(way, chunk, block).start()

    tile = min(256, hidden.shape[1])
    norm_rows = 16

    def feed(batch):
        def arrive(index, carry):
            chunk = batch * per + index // count
            block = index % count
            first = block == 0
            final = block == count - 1
            taken = jnp.logical_or(
                jnp.logical_and(first, relays(0)), jnp.logical_and(final, relays(1))
            )

            @pl.when(jnp.logical_and(crosses(block), jnp.logical_not(taken)))
            def _():
                cross(chunk, 1 - row, block).wait_recv()

            for end in (0, 1):

                @pl.when(
                    jnp.logical_and(
                        final if end else first,
                        jnp.logical_not(jnp.logical_or(crosses(block), taken)),
                    )
                )
                def _():
                    relay(end, chunk).wait_recv()

            return carry

        lax.fori_loop(0, per * count, arrive, 0)
        strips = rows // norm_rows

        def normalize(index, carry):
            slab = index // strips
            start = pl.multiple_of(index % strips * norm_rows, norm_rows)
            values = group[
                batch * per + slab // 2, slab % 2, pl.ds(start, norm_rows), :
            ].astype(jnp.float32)
            mean_square = jnp.mean(values * values, axis=1, keepdims=True)
            normed[pl.ds(pl.multiple_of(index * norm_rows, norm_rows), norm_rows), :] = (
                values
                * lax.rsqrt(mean_square + epsilon)
                * gains_ref[8:9, :].astype(jnp.float32)
            ).astype(jnp.bfloat16)
            return carry

        lax.fori_loop(0, 2 * per * strips, normalize, 0)

        @pl.when(batch == 0)
        def _():
            for load in loads:
                load.wait()

        def gated(index, carry):
            cut = pl.ds(pl.multiple_of(index * tile, tile), tile)
            gate_act = jnp.dot(normed[...], gate[:, cut], preferred_element_type=jnp.float32)
            up_act = jnp.dot(normed[...], up[:, cut], preferred_element_type=jnp.float32)
            hidden[:, cut] = (jax.nn.gelu(gate_act, approximate=True) * up_act).astype(
                jnp.bfloat16
            )
            return carry

        lax.fori_loop(0, hidden.shape[1] // tile, gated, 0)

        def contract(index, carry):
            step = count - 1 - index // 2
            rightward = index % 2 == 0
            block = jnp.where(rightward, me + step, me - step)
            inside = jnp.logical_and(block >= 0, block < count)

            @pl.when(jnp.logical_and(inside, jnp.logical_or(step > 0, rightward)))
            def _():
                pair[...] = jnp.dot(
                    hidden[...], down[:, columns(block)], preferred_element_type=jnp.float32
                ).reshape(per, 2, rows, width)
                for sub in range(per):
                    chunk = batch * per + sub
                    y_out[chunk, block] = pair[sub, 1 - row].astype(jnp.bfloat16)
                    across(chunk, block).start()
                    kept[chunk, block] = pair[sub, row]

            return carry

        lax.fori_loop(0, 2 * count, contract, 0)

    def tick(time, carry):
        def active(since):
            return jnp.logical_and(
                since % spacing == 0, jnp.logical_and(since >= 0, since < spacing * chunks)
            )

        def attention_turn(index, inner):
            since = time - (count - 1) + index

            @pl.when(active(since))
            def _():
                chain(attention_line, since // spacing, index, False)

            return inner

        def spread_turn(index, inner):
            hop_index = count - 1 - index
            since = time - (count - 1) - hop_index

            @pl.when(active(since))
            def _():
                spread(since // spacing, hop_index)

            return inner

        def hidden_turn(index, inner):
            since = time - hidden_base - (count - 1) + index

            @pl.when(active(since))
            def _():
                chain(hidden_line, since // spacing, index, True)

            return inner

        def relay_all():
            for end in (0, 1):
                turn = relay_turn(end)
                since = time - relay_base - turn
                chunk = since // spacing

                @pl.when(jnp.logical_and(relays(end), active(since)))
                def _():
                    @pl.when(turn == 0)
                    def _():
                        cross(chunk, 1 - row, end * (count - 1)).wait_recv()

                    @pl.when(turn > 0)
                    def _():
                        relay(end, chunk).wait_recv()

                    relay(end, chunk).start()

        def feed_turn():
            since = time - feed_base

            @pl.when(
                jnp.logical_and(
                    since % (spacing * per) == 0,
                    jnp.logical_and(since >= 0, since < spacing * chunks),
                )
            )
            def _():
                feed(since // (spacing * per))

        lax.fori_loop(0, count - 1, spread_turn, 0)
        lax.fori_loop(0, count, hidden_turn, 0)
        lax.fori_loop(0, count, attention_turn, 0)
        relay_all()
        feed_turn()
        return carry

    feed_base = 2 * count
    hidden_base = feed_base + 1
    relay_base = 2 * count - middle
    lax.fori_loop(0, spacing * (chunks - 1) + hidden_base + count, tick, 0)

    def drain(index, carry):
        chunk = index // count
        block = index % count
        across(chunk, block).wait_send()

        @pl.when(crosses(block))
        def _():
            cross(chunk, row, block).wait_send()

        for end in (0, 1):

            @pl.when(jnp.logical_and(block == end, relays(end)))
            def _():
                relay(end, chunk).wait_send()

        @pl.when(block > me)
        def _():
            hop(*attention_line, chunk, block, True).wait_send()
            hop(*hidden_line, chunk, block, True).wait_send()

        @pl.when(block < me)
        def _():
            hop(*attention_line, chunk, block, False).wait_send()
            hop(*hidden_line, chunk, block, False).wait_send()

        @pl.when(jnp.logical_and(me < count - 1, block <= me))
        def _():
            pass_on(0, chunk, block).wait_send()

        @pl.when(jnp.logical_and(me > 0, block >= me))
        def _():
            pass_on(1, chunk, block).wait_send()

        return carry

    lax.fori_loop(0, chunks * count, drain, 0)


def back(share, gains, tok, gate, up, down, count, chunks, collective_id):
    length, width = tok.shape
    rows = length // chunks
    per, spacing = 1, 2
    inner = down.shape[0]
    dma = pltpu.SemaphoreType.DMA
    vmem = pl.BlockSpec(memory_space=pltpu.VMEM)
    anywhere = pl.BlockSpec(memory_space=pl.ANY)
    line = pltpu.VMEM((chunks, count, rows, width), jnp.bfloat16)
    longer = pltpu.VMEM((chunks, count + 1, rows, width), jnp.bfloat16)
    return pl.pallas_call(
        functools.partial(back_kernel, count, chunks, per, spacing),
        out_shape=jax.ShapeDtypeStruct((length, width), jnp.bfloat16),
        in_specs=[vmem, vmem, vmem] + [anywhere] * 3,
        out_specs=vmem,
        scratch_shapes=[
            pltpu.VMEM(gate.shape, jnp.bfloat16),
            pltpu.VMEM(up.shape, jnp.bfloat16),
            pltpu.VMEM(down.shape, jnp.bfloat16),
            pltpu.VMEM((chunks, 2, rows, count * width), jnp.bfloat16),
            pltpu.VMEM((2 * per * rows, count * width), jnp.bfloat16),
            pltpu.VMEM((2 * per * rows, inner), jnp.bfloat16),
            pltpu.VMEM((per, 2, rows, width), jnp.float32),
            pltpu.VMEM((chunks, count, rows, width), jnp.float32),
            pltpu.VMEM((rows, width), jnp.float32),
            line,
            longer,
            line,
            longer,
            line,
            line,
            dma((3,)),
            dma((chunks, count)),
            dma((chunks, count + 1)),
            dma((chunks, count)),
            dma((chunks, count + 1)),
            dma((chunks, count)),
            dma((chunks, count)),
            dma((2, chunks, count)),
            dma((chunks, count)),
            dma((chunks, count)),
            dma((chunks, count)),
            dma((2, chunks)),
            dma((2, chunks)),
        ],
        compiler_params=pltpu.CompilerParams(
            collective_id=collective_id, has_side_effects=True, vmem_limit_bytes=60 * 2**20
        ),
    )(share, gains, tok, gate, up, down)


def on_device(
    tokens,
    attn_gain,
    query_weight,
    key_weight,
    value_projection_matrix,
    attention_output_matrix,
    bucket_bias_matrix,
    ffn_gain,
    gate_weight,
    up_weight,
    down_projection_weight,
):
    sequences, length, part_width = tokens.shape
    ma_count = lax.axis_size("ma")
    slab_rows = sequences * length
    token_rows = tokens.reshape(slab_rows, part_width)
    share, gains = front(
        token_rows,
        attn_gain,
        ffn_gain,
        bucket_bias_matrix,
        query_weight,
        key_weight,
        value_projection_matrix,
        attention_output_matrix,
        ma_count,
        3,
    )
    encoded = back(
        share,
        gains,
        token_rows,
        gate_weight,
        up_weight,
        down_projection_weight,
        ma_count,
        4,
        1,
    )
    return encoded.reshape(sequences, length, part_width)


def solution(mesh):
    in_specs = (
        P(("ba", "row"), None, "ma"),
        P("ma"),
        P("row", "ma"),
        P("row", "ma"),
        P("row", "ma"),
        P("ma", "row"),
        P(None, "ma"),
        P("ma"),
        P(None, ("ma", "row")),
        P(None, ("ma", "row")),
        P(("ma", "row"), None),
    )
    out_specs = P(("ba", "row"), None, "ma")
    return jax.shard_map(
        on_device, mesh=mesh, in_specs=in_specs, out_specs=out_specs, check_vma=False
    )
```

```python
import functools

import jax
import jax.numpy as jnp
from jax import lax
from jax.experimental import pallas as pl
from jax.experimental.pallas import tpu as pltpu
from jax.sharding import PartitionSpec as P

bucket_thresholds = (1, 2, 3, 4, 5, 6, 7, 8, 11, 16, 23, 32, 45, 64, 91, 128)
epsilon = 1e-06


MESH = pl.DeviceIdType.MESH


def layer_kernel(
    count,
    halves,
    groups,
    chunks,
    per,
    spacing,
    tok_ref,
    attn_gain_ref,
    ffn_gain_ref,
    table_ref,
    wq_ref,
    wk_ref,
    wv_ref,
    wo_ref,
    gate_ref,
    up_ref,
    down_ref,
    out_ref,
    qkv,
    up,
    out_full,
    gains,
    xs,
    scaled,
    part_out,
    part_in,
    sums_out,
    sums_in,
    lines,
    gain_tile,
    att,
    share,
    group,
    normed,
    hidden,
    pair,
    bias,
    kept,
    total,
    c_out,
    c_in,
    e_in,
    y_out,
    y_in,
    w_sem,
    d_sem,
    own_sem,
    gain_sem,
    wo_sem,
    g_send,
    g_recv,
    y_send,
    y_recv,
    z_send,
    z_recv,
    p_send,
    p_recv,
    s_send,
    s_recv,
    wy_send,
    wy_recv,
    wf_send,
    wf_recv,
    c_send,
    c_recv,
    e_send,
    e_recv,
    a_send,
    a_recv,
    d_send,
    d_recv,
    x_send,
    x_recv,
    r_send,
    r_recv,
):
    rows = tok_ref.shape[0] // chunks
    per_tile = bias.shape[3] // tok_ref.shape[0]
    gate = qkv.at[pl.ds(0, gate_ref.shape[0]), :]
    down = out_full
    me = lax.axis_index("ma")
    row = lax.axis_index("row")
    ba = lax.axis_index("ba")
    length, width = tok_ref.shape
    half_blocks = count // 2
    half = half_blocks * width
    inner = qkv.shape[1]
    heads = table_ref.shape[1]
    head_size = inner // heads
    half_rows = length // halves
    group_width = inner // groups
    home = me // half_blocks == row
    col_half = wo_ref.shape[1]
    pieces = wy_send.shape[0]
    lane_rows = wo_ref.shape[0] // 4
    piece_rows = lane_rows // pieces
    lane = ba % 4

    barrier = pltpu.get_barrier_semaphore()

    def hello(offset, carry):
        pl.semaphore_signal(
            barrier, inc=1, device_id={"ma": (me + offset) % count}, device_id_type=MESH
        )
        return carry

    lax.fori_loop(1, count, hello, 0)
    pl.semaphore_signal(barrier, inc=1, device_id={"row": 1 - row}, device_id_type=MESH)
    for flip in (1, 2, 3):
        pl.semaphore_signal(barrier, inc=1, device_id={"ba": ba ^ flip}, device_id_type=MESH)
    pl.semaphore_wait(barrier, count + 3)

    def place(seq, chunk, slot):
        return xs.at[
            seq,
            pl.ds(chunk * half_rows, half_rows),
            pl.ds(pl.multiple_of(slot * width, width), width),
        ]

    def z_copy(way, seq, chunk, block, src=None):
        slot = block - row * half_blocks
        here = place(seq, chunk, slot)
        return pltpu.make_async_remote_copy(
            src_ref=here if src is None else src,
            dst_ref=here,
            send_sem=z_send.at[way, seq, chunk, slot],
            recv_sem=z_recv.at[seq, chunk, slot],
            device_id={"ma": me + 1 - 2 * way},
            device_id_type=MESH,
        )

    def own(chunk):
        return tok_ref.at[pl.ds(chunk * half_rows, half_rows), :]

    def y_copy(chunk):
        return pltpu.make_async_remote_copy(
            src_ref=own(chunk),
            dst_ref=place(row, chunk, me - (1 - row) * half_blocks),
            send_sem=y_send.at[chunk],
            recv_sem=y_recv.at[chunk],
            device_id={"row": 1 - row},
            device_id_type=MESH,
        )

    def y_arrival(chunk):
        here = place(1 - row, chunk, me - row * half_blocks)
        return pltpu.make_async_remote_copy(
            src_ref=here,
            dst_ref=here,
            send_sem=y_send.at[chunk],
            recv_sem=y_recv.at[chunk],
            device_id={"row": 1 - row},
            device_id_type=MESH,
        )

    def launch(mine, chunk):
        seq = row if mine else 1 - row
        src = own(chunk) if mine else None

        @pl.when(home)
        def _():
            if not mine:
                y_arrival(chunk).wait_recv()

            @pl.when(me < count - 1)
            def _():
                z_copy(0, seq, chunk, me, src).start()

            @pl.when(me > 0)
            def _():
                z_copy(1, seq, chunk, me, src).start()

    def token_spread(mine, chunk):
        seq = row if mine else 1 - row

        def turn(step, carry):
            for way in (0, 1):
                block = me - step if way == 0 else me + step
                inside = jnp.logical_and(
                    block >= row * half_blocks, block < (row + 1) * half_blocks
                )

                @pl.when(inside)
                def _():
                    z_copy(way, seq, chunk, block).wait_recv()

                    @pl.when(me < count - 1 if way == 0 else me > 0)
                    def _():
                        z_copy(way, seq, chunk, block).start()

            return carry

        lax.fori_loop(1, count, turn, 0)

    def own_place():
        return xs.at[
            row, :, pl.ds(pl.multiple_of((me - row * half_blocks) * width, width), width)
        ]

    def gain_columns(block):
        return gains.at[:, pl.ds(pl.multiple_of(block * width, width), width)]

    def gain_copy(offset):
        return pltpu.make_async_remote_copy(
            src_ref=gain_tile,
            dst_ref=gain_columns(me),
            send_sem=g_send.at[offset],
            recv_sem=g_recv.at[me],
            device_id={"ma": (me + offset) % count},
            device_id_type=MESH,
        )

    def gain_arrival(block):
        return pltpu.make_async_remote_copy(
            src_ref=gain_tile,
            dst_ref=gain_columns(block),
            send_sem=g_send.at[0],
            recv_sem=g_recv.at[block],
            device_id={"ma": (me + 1) % count},
            device_id_type=MESH,
        )

    def wo_region(owner, piece, side):
        start = pl.multiple_of(owner * lane_rows + piece * piece_rows, piece_rows)
        return out_full.at[
            pl.ds(start, piece_rows), pl.ds(pl.multiple_of(side * col_half, col_half), col_half)
        ]

    def wo_y(piece):
        start = pl.multiple_of(lane * lane_rows + piece * piece_rows, piece_rows)
        return pltpu.make_async_remote_copy(
            src_ref=wo_ref.at[pl.ds(start, piece_rows), :],
            dst_ref=wo_region(lane, piece, row),
            send_sem=wy_send.at[piece],
            recv_sem=wy_recv.at[piece],
            device_id={"row": 1 - row},
            device_id_type=MESH,
        )

    def wo_y_arrival(piece):
        here = wo_region(lane, piece, 1 - row)
        return pltpu.make_async_remote_copy(
            src_ref=here,
            dst_ref=here,
            send_sem=wy_send.at[piece],
            recv_sem=wy_recv.at[piece],
            device_id={"row": 1 - row},
            device_id_type=MESH,
        )

    def wo_fan(flip, piece, owner):
        here = wo_region(owner, piece, 1 - row)
        return pltpu.make_async_remote_copy(
            src_ref=here,
            dst_ref=here,
            send_sem=wf_send.at[flip - 1, piece],
            recv_sem=wf_recv.at[flip - 1, piece],
            device_id={"ba": ba ^ flip},
            device_id_type=MESH,
        )

    def part_copy(chunk, group):
        return pltpu.make_async_remote_copy(
            src_ref=part_out.at[chunk, group],
            dst_ref=part_in.at[chunk, group],
            send_sem=p_send.at[chunk, group],
            recv_sem=p_recv.at[chunk, group],
            device_id={"row": 1 - row},
            device_id_type=MESH,
        )

    def sum_copy(chunk):
        return pltpu.make_async_remote_copy(
            src_ref=sums_out.at[chunk],
            dst_ref=sums_in.at[chunk],
            send_sem=s_send.at[chunk],
            recv_sem=s_recv.at[chunk],
            device_id={"row": 1 - row},
            device_id_type=MESH,
        )

    launch(True, 0)

    @pl.when(jnp.logical_not(home))
    def _():
        for chunk in range(halves):
            y_copy(chunk).start()

    for piece in range(pieces):
        wo_y(piece).start()

    half_lines = lax.broadcasted_iota(jnp.int32, gain_tile.shape, 0) < 8
    gain_tile[...] = jnp.where(
        half_lines,
        jnp.broadcast_to(attn_gain_ref[...].astype(jnp.float32)[None, :], gain_tile.shape),
        jnp.broadcast_to(ffn_gain_ref[...].astype(jnp.float32)[None, :], gain_tile.shape),
    ).astype(jnp.bfloat16)

    def gain_send(offset, carry):
        gain_copy(offset).start()
        return carry

    lax.fori_loop(1, count, gain_send, 0)
    gain_local = pltpu.make_async_copy(gain_tile, gain_columns(me), gain_sem)
    gain_local.start()
    own_local = pltpu.make_async_copy(tok_ref, own_place(), own_sem)

    @pl.when(home)
    def _():
        own_local.start()

    wo_local = pltpu.make_async_copy(
        wo_ref,
        out_full.at[:, pl.ds(pl.multiple_of(row * col_half, col_half), col_half)],
        wo_sem,
    )
    loads = [
        pltpu.make_async_copy(matrix, qkv.at[pl.ds(index * half, half), :], w_sem.at[index])
        for index, matrix in enumerate((wq_ref, wk_ref, wv_ref))
    ]
    for load in loads:
        load.start()
    wo_local.start()

    span = 2 * length
    offset = lax.broadcasted_iota(jnp.int32, (8, span), 1) - (length - 1)
    distance = jnp.abs(offset)
    backward = jnp.zeros_like(distance)
    for threshold in bucket_thresholds[:15]:
        backward = backward + (distance >= threshold).astype(jnp.int32)
    forward = jnp.full_like(distance, 15)
    for threshold in bucket_thresholds:
        forward = forward + (distance >= threshold).astype(jnp.int32)
    bucket = jnp.where(offset > 0, forward, backward)

    entries = lax.broadcasted_iota(jnp.int32, (table_ref.shape[0], span), 0)
    chosen = (entries == jnp.broadcast_to(bucket[0:1, :], entries.shape)).astype(jnp.float32)
    lines[...] = lax.dot_general(
        table_ref[...],
        chosen,
        (((0,), (0,)), ((), ())),
        precision=lax.Precision.HIGHEST,
        preferred_element_type=jnp.float32,
    )

    def build_bias(head, carry):
        tile = jnp.broadcast_to(lines[pl.ds(head, 1), :], (length, span))
        tile = pltpu.roll(tile, length + 1, 1, stride=1, stride_axis=0)
        for chunk in range(chunks):
            bias[
                chunk,
                head // per_tile,
                :,
                pl.ds(pl.multiple_of(head % per_tile * length, length), length),
            ] = tile[chunk * rows : (chunk + 1) * rows, :length]
        return carry

    lax.fori_loop(0, heads, build_bias, 0)
    gain_local.wait()

    @pl.when(home)
    def _():
        own_local.wait()

    def gain_wait(step, carry):
        gain_arrival((me + step) % count).wait_recv()
        return carry

    lax.fori_loop(1, count, gain_wait, 0)
    gain_half = gains[
        pl.ds(0, 8), pl.ds(pl.multiple_of(row * half, half), half)
    ][0:1, :].astype(jnp.float32)

    def multiply_gain(seq, start, size):
        values = xs[seq, pl.ds(start, size), :].astype(jnp.float32)
        scaled[pl.ds(start, size), :] = (values * gain_half).astype(jnp.bfloat16)
        return jnp.sum(values * values, axis=1, keepdims=True)

    def outgoing(chunk):
        squares = multiply_gain(1 - row, chunk * half_rows, half_rows)
        for start in range(0, half_rows, 128):
            sums_out[chunk, :, start : start + 128] = jnp.broadcast_to(
                squares[start : start + 128], (128, 128)
            ).T[0:8]
        sum_copy(chunk).start()

        def turn(group, carry):
            columns = pl.ds(pl.multiple_of(group * group_width, group_width), group_width)
            for index in range(3):
                part_out[chunk, group, :, pl.ds(index * group_width, group_width)] = jnp.dot(
                    scaled[pl.ds(chunk * half_rows, half_rows), :],
                    qkv[pl.ds(index * half, half), columns],
                    preferred_element_type=jnp.float32,
                ).astype(jnp.bfloat16)
            part_copy(chunk, group).start()
            return carry

        lax.fori_loop(0, groups, turn, 0)

    def fan(piece):
        wo_y_arrival(piece).wait_recv()
        for flip in (1, 2, 3):
            wo_fan(flip, piece, lane).start()

    token_spread(True, 0)
    launch(False, 0)
    fan(0)
    token_spread(False, 0)
    launch(False, 1)
    for load in loads:
        load.wait()
    fan(1)
    outgoing(0)
    token_spread(False, 1)
    launch(True, 1)
    fan(2)
    outgoing(1)
    fan(3)
    token_spread(True, 1)
    own_squares = multiply_gain(row, 0, length)
    for chunk in range(halves):
        sum_copy(chunk).wait_recv()
    other_squares = jnp.concatenate(
        [
            jnp.broadcast_to(sums_in[chunk, 0:1, start : start + 128], (128, 128)).T[:, 0:1]
            for chunk in range(halves)
            for start in range(0, half_rows, 128)
        ]
    )
    scale = lax.rsqrt((own_squares + other_squares) / (count * width) + epsilon)
    members = 128 // head_size
    first_lanes = lax.broadcasted_iota(jnp.int32, (length, 128), 1)

    def bias_of(head):
        lanes = pl.ds(pl.multiple_of(head % per_tile * length, length), length)
        return jnp.concatenate(
            [bias[chunk, head // per_tile, :, lanes] for chunk in range(chunks)]
        )

    def attend(member_group, carry):
        columns = pl.ds(pl.multiple_of(member_group * group_width, group_width), group_width)
        products = [
            jnp.dot(scaled[...], qkv[pl.ds(index * half, half), columns], preferred_element_type=jnp.float32)
            for index in range(3)
        ]
        for chunk in range(halves):
            part_copy(chunk, member_group).wait_recv()
        query, key, value = [
            (
                (
                    product
                    + part_in[:, member_group, :, pl.ds(index * group_width, group_width)]
                    .astype(jnp.float32)
                    .reshape(length, group_width)
                )
                * scale
            ).astype(jnp.bfloat16)
            for index, product in enumerate(products)
        ]
        for tile in range(group_width // 128):
            cut = slice(tile * 128, (tile + 1) * 128)
            query_pair, key_pair, value_pair = query[:, cut], key[:, cut], value[:, cut]
            outcome = None
            for member in range(members):
                mask = jnp.logical_and(
                    first_lanes >= member * head_size, first_lanes < (member + 1) * head_size
                )
                scores = (
                    lax.dot_general(
                        jnp.where(mask, query_pair.astype(jnp.float32), 0.0).astype(jnp.bfloat16),
                        key_pair,
                        (((1,), (1,)), ((), ())),
                        preferred_element_type=jnp.float32,
                    )
                    + bias_of(member_group * (group_width // head_size) + tile * members + member)
                )
                exponent = jnp.exp(scores - jnp.max(scores, axis=1, keepdims=True))
                total = jnp.sum(exponent, axis=1, keepdims=True)
                mixed = jnp.dot(
                    (exponent / total).astype(jnp.bfloat16),
                    value_pair,
                    preferred_element_type=jnp.float32,
                )
                outcome = mixed if outcome is None else jnp.where(mask, mixed, outcome)
            att[
                :, pl.ds(pl.multiple_of(member_group * group_width + tile * 128, 128), 128)
            ] = outcome.astype(jnp.bfloat16)
        return carry

    lax.fori_loop(0, groups, attend, 0)

    later = [
        pltpu.make_async_copy(gate_ref, gate, d_sem.at[0]),
        pltpu.make_async_copy(up_ref, up, d_sem.at[1]),
        pltpu.make_async_copy(down_ref, down, d_sem.at[2]),
    ]
    later[0].start()
    later[1].start()
    wo_local.wait()
    for piece in range(pieces):
        for flip in (1, 2, 3):
            wo_fan(flip, piece, lane ^ flip).wait_recv()

    def project(block, carry):
        columns = pl.ds(pl.multiple_of(block * width, width), width)
        share[block] = jnp.dot(
            att[...], out_full[:, columns], preferred_element_type=jnp.float32
        ).astype(jnp.bfloat16)
        return carry

    lax.fori_loop(0, count, project, 0)
    for piece in range(pieces):
        wo_y(piece).wait_send()
        for flip in (1, 2, 3):
            wo_fan(flip, piece, lane).wait_send()
    later[2].start()

    def columns(block):
        return pl.ds(pl.multiple_of(block * width, width), width)

    def chunk_rows(chunk):
        return pl.ds(pl.multiple_of(chunk * rows, rows), rows)

    def hop(outs, ins, sends, recvs, chunk, block, rightward):
        slot = block if rightward else jnp.where(block == me - 1, count, block)
        return pltpu.make_async_remote_copy(
            src_ref=outs.at[chunk, block],
            dst_ref=ins.at[chunk, slot],
            send_sem=sends.at[chunk, block],
            recv_sem=recvs.at[chunk, slot],
            device_id={"ma": me + 1 if rightward else me - 1},
            device_id_type=MESH,
        )

    def landed(outs, ins, sends, recvs, chunk, slot, from_left):
        return pltpu.make_async_remote_copy(
            src_ref=outs.at[chunk, 0],
            dst_ref=ins.at[chunk, slot],
            send_sem=sends.at[chunk, 0],
            recv_sem=recvs.at[chunk, slot],
            device_id={"ma": me - 1 if from_left else me + 1},
            device_id_type=MESH,
        )

    def across(chunk, block):
        return pltpu.make_async_remote_copy(
            src_ref=y_out.at[chunk, block],
            dst_ref=y_in.at[chunk, block],
            send_sem=a_send.at[chunk, block],
            recv_sem=a_recv.at[chunk, block],
            device_id={"row": 1 - row},
            device_id_type=MESH,
        )

    def spot(chunk, seq, block):
        return group.at[chunk, seq, :, columns(block)]

    def pass_on(way, chunk, block):
        here = spot(chunk, row, block)
        return pltpu.make_async_remote_copy(
            src_ref=here,
            dst_ref=here,
            send_sem=d_send.at[way, chunk, block],
            recv_sem=d_recv.at[chunk, block],
            device_id={"ma": me + 1 - 2 * way},
            device_id_type=MESH,
        )

    def cross(chunk, seq, block):
        here = spot(chunk, seq, block)
        return pltpu.make_async_remote_copy(
            src_ref=here,
            dst_ref=here,
            send_sem=x_send.at[chunk, block],
            recv_sem=x_recv.at[chunk, block],
            device_id={"row": 1 - row},
            device_id_type=MESH,
        )

    middle = count // 2

    def crosses(block):
        return jnp.logical_not(
            jnp.logical_or(
                jnp.logical_and(block == 0, me >= middle),
                jnp.logical_and(block == count - 1, me < middle),
            )
        )

    def relay(end, chunk):
        here = spot(chunk, 1 - row, end * (count - 1))
        return pltpu.make_async_remote_copy(
            src_ref=here,
            dst_ref=here,
            send_sem=r_send.at[end, chunk],
            recv_sem=r_recv.at[end, chunk],
            device_id={"ma": me + 1 - 2 * end},
            device_id_type=MESH,
        )

    def relay_turn(end):
        return me - (middle - 1) if end == 0 else middle - me

    def relays(end):
        turn = relay_turn(end)
        return jnp.logical_and(turn >= 0, turn < middle)

    def residual(chunk):
        group[chunk, row, :, columns(me)] = (
            tok_ref[chunk_rows(chunk), :].astype(jnp.float32) + total[...]
        ).astype(jnp.bfloat16)
        cross(chunk, row, me).start()

        @pl.when(me < count - 1)
        def _():
            pass_on(0, chunk, me).start()

        @pl.when(me > 0)
        def _():
            pass_on(1, chunk, me).start()

    def encode(chunk):
        out_ref[chunk_rows(chunk), :] = (
            group[chunk, row, :, columns(me)].astype(jnp.float32) + total[...]
        ).astype(jnp.bfloat16)

    attention_line = (c_out, c_in, c_send, c_recv)
    hidden_line = (c_out, e_in, e_send, e_recv)

    def chain(line, chunk, step, last):
        outs, ins, sends, recvs = line
        for rightward in (True, False):
            block = me + step if rightward else me - step
            inside = jnp.logical_and(block >= 0, block < count)
            if not rightward:
                inside = jnp.logical_and(inside, step > 0)

            @pl.when(inside)
            def _():
                if last:
                    across(chunk, block).wait_recv()
                    total[...] = kept[chunk, block] + y_in[chunk, block].astype(jnp.float32)
                else:
                    total[...] = share[block, chunk_rows(chunk), :].astype(jnp.float32)

                if rightward:

                    @pl.when(me > 0)
                    def _():
                        landed(*line, chunk, block, True).wait_recv()
                        total[...] = total[...] + ins[chunk, block].astype(jnp.float32)

                    @pl.when(jnp.logical_and(step == 0, me < count - 1))
                    def _():
                        landed(*line, chunk, count, False).wait_recv()
                        total[...] = total[...] + ins[chunk, count].astype(jnp.float32)

                    @pl.when(step == 0)
                    def _():
                        if last:
                            encode(chunk)
                        else:
                            residual(chunk)

                    @pl.when(step > 0)
                    def _():
                        if last:
                            hop(*attention_line, chunk, block, True).wait_send()
                        outs[chunk, block] = total[...].astype(jnp.bfloat16)
                        hop(*line, chunk, block, True).start()

                else:

                    @pl.when(me < count - 1)
                    def _():
                        landed(*line, chunk, block, False).wait_recv()
                        total[...] = total[...] + ins[chunk, block].astype(jnp.float32)

                    if last:
                        hop(*attention_line, chunk, block, False).wait_send()
                    outs[chunk, block] = total[...].astype(jnp.bfloat16)
                    hop(*line, chunk, block, False).start()

    def spread(chunk, step):
        for way in (0, 1):
            block = me - step if way == 0 else me + step

            @pl.when(jnp.logical_and(block >= 0, block < count))
            def _():
                pass_on(way, chunk, block).wait_recv()

                @pl.when(crosses(block))
                def _():
                    cross(chunk, row, block).start()

                @pl.when(me < count - 1 if way == 0 else me > 0)
                def _():
                    pass_on(way, chunk, block).start()

    tile = min(256, hidden.shape[1])
    norm_rows = 16

    def feed(batch):
        def arrive(index, carry):
            chunk = batch * per + index // count
            block = index % count
            first = block == 0
            final = block == count - 1
            taken = jnp.logical_or(
                jnp.logical_and(first, relays(0)), jnp.logical_and(final, relays(1))
            )

            @pl.when(jnp.logical_and(crosses(block), jnp.logical_not(taken)))
            def _():
                cross(chunk, 1 - row, block).wait_recv()

            for end in (0, 1):

                @pl.when(
                    jnp.logical_and(
                        final if end else first,
                        jnp.logical_not(jnp.logical_or(crosses(block), taken)),
                    )
                )
                def _():
                    relay(end, chunk).wait_recv()

            return carry

        lax.fori_loop(0, per * count, arrive, 0)
        strips = rows // norm_rows

        def normalize(index, carry):
            slab = index // strips
            start = pl.multiple_of(index % strips * norm_rows, norm_rows)
            values = group[
                batch * per + slab // 2, slab % 2, pl.ds(start, norm_rows), :
            ].astype(jnp.float32)
            mean_square = jnp.mean(values * values, axis=1, keepdims=True)
            normed[pl.ds(pl.multiple_of(index * norm_rows, norm_rows), norm_rows), :] = (
                values
                * lax.rsqrt(mean_square + epsilon)
                * gains[8:9, :].astype(jnp.float32)
            ).astype(jnp.bfloat16)
            return carry

        lax.fori_loop(0, 2 * per * strips, normalize, 0)

        @pl.when(batch == 0)
        def _():
            for load in later:
                load.wait()

        def gated(index, carry):
            cut = pl.ds(pl.multiple_of(index * tile, tile), tile)
            gate_act = jnp.dot(normed[...], gate[:, cut], preferred_element_type=jnp.float32)
            up_act = jnp.dot(normed[...], up[:, cut], preferred_element_type=jnp.float32)
            hidden[:, cut] = (jax.nn.gelu(gate_act, approximate=True) * up_act).astype(
                jnp.bfloat16
            )
            return carry

        lax.fori_loop(0, hidden.shape[1] // tile, gated, 0)

        def contract(index, carry):
            step = count - 1 - index // 2
            rightward = index % 2 == 0
            block = jnp.where(rightward, me + step, me - step)
            inside = jnp.logical_and(block >= 0, block < count)

            @pl.when(jnp.logical_and(inside, jnp.logical_or(step > 0, rightward)))
            def _():
                pair[...] = jnp.dot(
                    hidden[...], down[:, columns(block)], preferred_element_type=jnp.float32
                ).reshape(per, 2, rows, width)
                for sub in range(per):
                    chunk = batch * per + sub
                    y_out[chunk, block] = pair[sub, 1 - row].astype(jnp.bfloat16)
                    across(chunk, block).start()
                    kept[chunk, block] = pair[sub, row]

            return carry

        lax.fori_loop(0, 2 * count, contract, 0)

    def tick(time, carry):
        def active(since):
            return jnp.logical_and(
                since % spacing == 0, jnp.logical_and(since >= 0, since < spacing * chunks)
            )

        def attention_turn(index, inner):
            since = time - (count - 1) + index

            @pl.when(active(since))
            def _():
                chain(attention_line, since // spacing, index, False)

            return inner

        def spread_turn(index, inner):
            hop_index = count - 1 - index
            since = time - (count - 1) - hop_index

            @pl.when(active(since))
            def _():
                spread(since // spacing, hop_index)

            return inner

        def hidden_turn(index, inner):
            since = time - hidden_base - (count - 1) + index

            @pl.when(active(since))
            def _():
                chain(hidden_line, since // spacing, index, True)

            return inner

        def relay_all():
            for end in (0, 1):
                turn = relay_turn(end)
                since = time - relay_base - turn
                chunk = since // spacing

                @pl.when(jnp.logical_and(relays(end), active(since)))
                def _():
                    @pl.when(turn == 0)
                    def _():
                        cross(chunk, 1 - row, end * (count - 1)).wait_recv()

                    @pl.when(turn > 0)
                    def _():
                        relay(end, chunk).wait_recv()

                    relay(end, chunk).start()

        def feed_turn():
            since = time - feed_base

            @pl.when(
                jnp.logical_and(
                    since % (spacing * per) == 0,
                    jnp.logical_and(since >= 0, since < spacing * chunks),
                )
            )
            def _():
                feed(since // (spacing * per))

        lax.fori_loop(0, count - 1, spread_turn, 0)
        lax.fori_loop(0, count, hidden_turn, 0)
        lax.fori_loop(0, count, attention_turn, 0)
        relay_all()
        feed_turn()
        return carry

    feed_base = 2 * count
    hidden_base = feed_base + 1
    relay_base = 2 * count - middle
    lax.fori_loop(0, spacing * (chunks - 1) + hidden_base + count, tick, 0)

    def drain(index, carry):
        chunk = index // count
        block = index % count
        across(chunk, block).wait_send()

        @pl.when(crosses(block))
        def _():
            cross(chunk, row, block).wait_send()

        for end in (0, 1):

            @pl.when(jnp.logical_and(block == end, relays(end)))
            def _():
                relay(end, chunk).wait_send()

        @pl.when(block > me)
        def _():
            hop(*hidden_line, chunk, block, True).wait_send()

        @pl.when(block < me)
        def _():
            hop(*hidden_line, chunk, block, False).wait_send()

        @pl.when(jnp.logical_and(me < count - 1, block <= me))
        def _():
            pass_on(0, chunk, block).wait_send()

        @pl.when(jnp.logical_and(me > 0, block >= me))
        def _():
            pass_on(1, chunk, block).wait_send()

        return carry

    lax.fori_loop(0, chunks * count, drain, 0)


    for chunk in range(halves):
        sum_copy(chunk).wait_send()

        def part_drain(group, carry):
            part_copy(chunk, group).wait_send()
            return carry

        lax.fori_loop(0, groups, part_drain, 0)

        @pl.when(jnp.logical_not(home))
        def _():
            y_copy(chunk).wait_send()

        def z_drain(slot, carry):
            block = slot + row * half_blocks
            for seq in (0, 1):

                @pl.when(jnp.logical_and(me < count - 1, block <= me))
                def _():
                    z_copy(0, seq, chunk, block).wait_send()

                @pl.when(jnp.logical_and(me > 0, block >= me))
                def _():
                    z_copy(1, seq, chunk, block).wait_send()

            return carry

        lax.fori_loop(0, half_blocks, z_drain, 0)

    def gain_drain(offset, carry):
        gain_copy(offset).wait_send()
        return carry

    lax.fori_loop(1, count, gain_drain, 0)


def layer(
    tok, attn_gain, ffn_gain, table, wq, wk, wv, wo, gate, up, down, count, collective_id
):
    length, width = tok.shape
    halves, chunks, per, spacing, pieces = 2, 4, 1, 2, 4
    inner = wq.shape[1]
    heads = table.shape[1]
    groups = max(1, inner // 256)
    half = wq.shape[0]
    half_rows = length // halves
    rows = length // chunks
    group_width = inner // groups
    per_tile = max(1, min(heads, width // length))
    dma = pltpu.SemaphoreType.DMA
    vmem = pl.BlockSpec(memory_space=pltpu.VMEM)
    anywhere = pl.BlockSpec(memory_space=pl.ANY)
    bf16 = lambda *shape: pltpu.VMEM(shape, jnp.bfloat16)
    f32 = lambda *shape: pltpu.VMEM(shape, jnp.float32)
    bias_shape = (chunks, heads // per_tile, rows, per_tile * length)
    kept_shape = (chunks, count, rows, width)
    shared = bias_shape == kept_shape

    def body(*refs):
        refs = list(refs)
        if shared:
            refs.insert(31, refs[30])
        layer_kernel(count, halves, groups, chunks, per, spacing, *refs)

    return pl.pallas_call(
        body,
        out_shape=jax.ShapeDtypeStruct((length, width), jnp.bfloat16),
        in_specs=[vmem] * 4 + [anywhere] * 7,
        out_specs=vmem,
        scratch_shapes=[
            bf16(3 * half, inner),
            bf16(*up.shape),
            bf16(wo.shape[0], 2 * wo.shape[1]),
            bf16(16, count * width),
            bf16(2, length, half),
            bf16(length, half),
            bf16(halves, groups, half_rows, 3 * group_width),
            bf16(halves, groups, half_rows, 3 * group_width),
            f32(halves, 8, half_rows),
            f32(halves, 8, half_rows),
            f32(heads, 2 * length),
            bf16(16, width),
            bf16(length, inner),
            bf16(count, length, width),
            bf16(chunks, 2, rows, count * width),
            bf16(2 * per * rows, count * width),
            bf16(2 * per * rows, down.shape[0]),
            f32(per, 2, rows, width),
            f32(*bias_shape),
        ]
        + ([] if shared else [f32(*kept_shape)])
        + [
            f32(rows, width),
            bf16(chunks, count, rows, width),
            bf16(chunks, count + 1, rows, width),
            bf16(chunks, count + 1, rows, width),
            bf16(chunks, count, rows, width),
            bf16(chunks, count, rows, width),
            dma((3,)),
            dma((3,)),
            dma,
            dma,
            dma,
            dma((count,)),
            dma((count,)),
            dma((halves,)),
            dma((halves,)),
            dma((2, 2, halves, count // 2)),
            dma((2, halves, count // 2)),
            dma((halves, groups)),
            dma((halves, groups)),
            dma((halves,)),
            dma((halves,)),
            dma((pieces,)),
            dma((pieces,)),
            dma((3, pieces)),
            dma((3, pieces)),
            dma((chunks, count)),
            dma((chunks, count + 1)),
            dma((chunks, count)),
            dma((chunks, count + 1)),
            dma((chunks, count)),
            dma((chunks, count)),
            dma((2, chunks, count)),
            dma((chunks, count)),
            dma((chunks, count)),
            dma((chunks, count)),
            dma((2, chunks)),
            dma((2, chunks)),
        ],
        compiler_params=pltpu.CompilerParams(
            collective_id=collective_id, has_side_effects=True, vmem_limit_bytes=67043328
        ),
    )(tok, attn_gain, ffn_gain, table, wq, wk, wv, wo, gate, up, down)


def on_device(
    tokens,
    attn_gain,
    query_weight,
    key_weight,
    value_projection_matrix,
    attention_output_matrix,
    bucket_bias_matrix,
    ffn_gain,
    gate_weight,
    up_weight,
    down_projection_weight,
):
    sequences, length, part_width = tokens.shape
    ma_count = lax.axis_size("ma")
    slab_rows = sequences * length
    token_rows = tokens.reshape(slab_rows, part_width)
    encoded = layer(
        token_rows,
        attn_gain,
        ffn_gain,
        bucket_bias_matrix,
        query_weight,
        key_weight,
        value_projection_matrix,
        attention_output_matrix,
        gate_weight,
        up_weight,
        down_projection_weight,
        ma_count,
        1,
    )
    return encoded.reshape(sequences, length, part_width)


def solution(mesh):
    in_specs = (
        P(("ba", "row"), None, "ma"),
        P("ma"),
        P("row", "ma"),
        P("row", "ma"),
        P("row", "ma"),
        P("ma", "row"),
        P(None, "ma"),
        P("ma"),
        P(None, ("ma", "row")),
        P(None, ("ma", "row")),
        P(("ma", "row"), None),
    )
    out_specs = P(("ba", "row"), None, "ma")
    return jax.shard_map(
        on_device, mesh=mesh, in_specs=in_specs, out_specs=out_specs, check_vma=False
    )
```

```python
import functools

import jax
import jax.numpy as jnp
from jax import lax
from jax.experimental import pallas as pl
from jax.experimental.pallas import tpu as pltpu
from jax.sharding import PartitionSpec as P

bucket_thresholds = (1, 2, 3, 4, 5, 6, 7, 8, 11, 16, 23, 32, 45, 64, 91, 128)
epsilon = 1e-06


MESH = pl.DeviceIdType.MESH


def layer_kernel(
    count,
    halves,
    groups,
    chunks,
    per,
    spacing,
    tok_ref,
    attn_gain_ref,
    ffn_gain_ref,
    table_ref,
    wq_ref,
    wk_ref,
    wv_ref,
    wo_ref,
    gate_ref,
    up_ref,
    down_ref,
    out_ref,
    qkv,
    up,
    out_full,
    gains,
    xs,
    scaled,
    part_out,
    part_in,
    sums_out,
    sums_in,
    lines,
    gain_tile,
    att,
    share,
    group,
    normed,
    hidden,
    pair,
    bias,
    kept,
    total,
    c_out,
    c_in,
    e_in,
    y_out,
    y_in,
    w_sem,
    d_sem,
    own_sem,
    gain_sem,
    wo_sem,
    g_send,
    g_recv,
    y_send,
    y_recv,
    z_send,
    z_recv,
    p_send,
    p_recv,
    s_send,
    s_recv,
    wy_send,
    wy_recv,
    wf_send,
    wf_recv,
    c_send,
    c_recv,
    e_send,
    e_recv,
    a_send,
    a_recv,
    d_send,
    d_recv,
    x_send,
    x_recv,
    r_send,
    r_recv,
):
    rows = tok_ref.shape[0] // chunks
    per_tile = bias.shape[3] // tok_ref.shape[0]
    gate = qkv.at[pl.ds(0, gate_ref.shape[0]), :]
    down = out_full
    me = lax.axis_index("ma")
    row = lax.axis_index("row")
    ba = lax.axis_index("ba")
    length, width = tok_ref.shape
    half_blocks = count // 2
    half = half_blocks * width
    inner = qkv.shape[1]
    heads = table_ref.shape[0]
    head_size = inner // heads
    half_rows = length // halves
    group_width = inner // groups
    home = me // half_blocks == row
    col_half = wo_ref.shape[1]
    pieces = wy_send.shape[0]
    lane_rows = wo_ref.shape[0] // 4
    piece_rows = lane_rows // pieces
    lane = ba % 4

    barrier = pltpu.get_barrier_semaphore()

    def hello(offset, carry):
        pl.semaphore_signal(
            barrier, inc=1, device_id={"ma": (me + offset) % count}, device_id_type=MESH
        )
        return carry

    lax.fori_loop(1, count, hello, 0)
    pl.semaphore_signal(barrier, inc=1, device_id={"row": 1 - row}, device_id_type=MESH)
    for flip in (1, 2, 3):
        pl.semaphore_signal(barrier, inc=1, device_id={"ba": ba ^ flip}, device_id_type=MESH)
    pl.semaphore_wait(barrier, count + 3)

    def place(seq, chunk, slot):
        return xs.at[
            seq,
            pl.ds(chunk * half_rows, half_rows),
            pl.ds(pl.multiple_of(slot * width, width), width),
        ]

    def z_copy(way, seq, chunk, block, src=None):
        slot = block - row * half_blocks
        here = place(seq, chunk, slot)
        return pltpu.make_async_remote_copy(
            src_ref=here if src is None else src,
            dst_ref=here,
            send_sem=z_send.at[way, seq, chunk, slot],
            recv_sem=z_recv.at[seq, chunk, slot],
            device_id={"ma": me + 1 - 2 * way},
            device_id_type=MESH,
        )

    def own(chunk):
        return tok_ref.at[pl.ds(chunk * half_rows, half_rows), :]

    def y_copy(chunk):
        return pltpu.make_async_remote_copy(
            src_ref=own(chunk),
            dst_ref=place(row, chunk, me - (1 - row) * half_blocks),
            send_sem=y_send.at[chunk],
            recv_sem=y_recv.at[chunk],
            device_id={"row": 1 - row},
            device_id_type=MESH,
        )

    def y_arrival(chunk):
        here = place(1 - row, chunk, me - row * half_blocks)
        return pltpu.make_async_remote_copy(
            src_ref=here,
            dst_ref=here,
            send_sem=y_send.at[chunk],
            recv_sem=y_recv.at[chunk],
            device_id={"row": 1 - row},
            device_id_type=MESH,
        )

    def launch(mine, chunk):
        seq = row if mine else 1 - row
        src = own(chunk) if mine else None

        @pl.when(home)
        def _():
            if not mine:
                y_arrival(chunk).wait_recv()

            @pl.when(me < count - 1)
            def _():
                z_copy(0, seq, chunk, me, src).start()

            @pl.when(me > 0)
            def _():
                z_copy(1, seq, chunk, me, src).start()

    def token_spread(mine, chunk):
        seq = row if mine else 1 - row

        def turn(step, carry):
            for way in (0, 1):
                block = me - step if way == 0 else me + step
                inside = jnp.logical_and(
                    block >= row * half_blocks, block < (row + 1) * half_blocks
                )

                @pl.when(inside)
                def _():
                    z_copy(way, seq, chunk, block).wait_recv()

                    @pl.when(me < count - 1 if way == 0 else me > 0)
                    def _():
                        z_copy(way, seq, chunk, block).start()

            return carry

        lax.fori_loop(1, count, turn, 0)

    def own_place():
        return xs.at[
            row, :, pl.ds(pl.multiple_of((me - row * half_blocks) * width, width), width)
        ]

    def gain_columns(block):
        return gains.at[:, pl.ds(pl.multiple_of(block * width, width), width)]

    def gain_copy(offset):
        return pltpu.make_async_remote_copy(
            src_ref=gain_tile,
            dst_ref=gain_columns(me),
            send_sem=g_send.at[offset],
            recv_sem=g_recv.at[me],
            device_id={"ma": (me + offset) % count},
            device_id_type=MESH,
        )

    def gain_arrival(block):
        return pltpu.make_async_remote_copy(
            src_ref=gain_tile,
            dst_ref=gain_columns(block),
            send_sem=g_send.at[0],
            recv_sem=g_recv.at[block],
            device_id={"ma": (me + 1) % count},
            device_id_type=MESH,
        )

    def wo_region(owner, piece, side):
        start = pl.multiple_of(owner * lane_rows + piece * piece_rows, piece_rows)
        return out_full.at[
            pl.ds(start, piece_rows), pl.ds(pl.multiple_of(side * col_half, col_half), col_half)
        ]

    def wo_y(piece):
        start = pl.multiple_of(lane * lane_rows + piece * piece_rows, piece_rows)
        return pltpu.make_async_remote_copy(
            src_ref=wo_ref.at[pl.ds(start, piece_rows), :],
            dst_ref=wo_region(lane, piece, row),
            send_sem=wy_send.at[piece],
            recv_sem=wy_recv.at[piece],
            device_id={"row": 1 - row},
            device_id_type=MESH,
        )

    def wo_y_arrival(piece):
        here = wo_region(lane, piece, 1 - row)
        return pltpu.make_async_remote_copy(
            src_ref=here,
            dst_ref=here,
            send_sem=wy_send.at[piece],
            recv_sem=wy_recv.at[piece],
            device_id={"row": 1 - row},
            device_id_type=MESH,
        )

    def wo_fan(flip, piece, owner):
        here = wo_region(owner, piece, 1 - row)
        return pltpu.make_async_remote_copy(
            src_ref=here,
            dst_ref=here,
            send_sem=wf_send.at[flip - 1, piece],
            recv_sem=wf_recv.at[flip - 1, piece],
            device_id={"ba": ba ^ flip},
            device_id_type=MESH,
        )

    def part_copy(chunk, group):
        return pltpu.make_async_remote_copy(
            src_ref=part_out.at[chunk, group],
            dst_ref=part_in.at[chunk, group],
            send_sem=p_send.at[chunk, group],
            recv_sem=p_recv.at[chunk, group],
            device_id={"row": 1 - row},
            device_id_type=MESH,
        )

    def sum_copy(chunk):
        return pltpu.make_async_remote_copy(
            src_ref=sums_out.at[chunk],
            dst_ref=sums_in.at[chunk],
            send_sem=s_send.at[chunk],
            recv_sem=s_recv.at[chunk],
            device_id={"row": 1 - row},
            device_id_type=MESH,
        )

    launch(True, 0)

    @pl.when(jnp.logical_not(home))
    def _():
        for chunk in range(halves):
            y_copy(chunk).start()

    for piece in range(pieces):
        wo_y(piece).start()

    half_lines = lax.broadcasted_iota(jnp.int32, gain_tile.shape, 0) < 8
    gain_tile[...] = jnp.where(
        half_lines,
        jnp.broadcast_to(attn_gain_ref[...].astype(jnp.float32)[None, :], gain_tile.shape),
        jnp.broadcast_to(ffn_gain_ref[...].astype(jnp.float32)[None, :], gain_tile.shape),
    ).astype(jnp.bfloat16)

    def gain_send(offset, carry):
        gain_copy(offset).start()
        return carry

    lax.fori_loop(1, count, gain_send, 0)
    gain_local = pltpu.make_async_copy(gain_tile, gain_columns(me), gain_sem)
    gain_local.start()
    own_local = pltpu.make_async_copy(tok_ref, own_place(), own_sem)

    @pl.when(home)
    def _():
        own_local.start()

    wo_local = pltpu.make_async_copy(
        wo_ref,
        out_full.at[:, pl.ds(pl.multiple_of(row * col_half, col_half), col_half)],
        wo_sem,
    )
    loads = [
        pltpu.make_async_copy(matrix, qkv.at[pl.ds(index * half, half), :], w_sem.at[index])
        for index, matrix in enumerate((wq_ref, wk_ref, wv_ref))
    ]
    for load in loads:
        load.start()
    wo_local.start()

    span = 2 * length
    offset = lax.broadcasted_iota(jnp.int32, (8, span), 1) - (length - 1)
    distance = jnp.abs(offset)
    backward = jnp.zeros_like(distance)
    for threshold in bucket_thresholds[:15]:
        backward = backward + (distance >= threshold).astype(jnp.int32)
    forward = jnp.full_like(distance, 15)
    for threshold in bucket_thresholds:
        forward = forward + (distance >= threshold).astype(jnp.int32)
    bucket = jnp.where(offset > 0, forward, backward)

    entries = lax.broadcasted_iota(jnp.int32, (table_ref.shape[1], span), 0)
    chosen = (entries == jnp.broadcast_to(bucket[0:1, :], entries.shape)).astype(jnp.float32)
    lines[...] = lax.dot_general(
        table_ref[...],
        chosen,
        (((1,), (0,)), ((), ())),
        precision=lax.Precision.HIGHEST,
        preferred_element_type=jnp.float32,
    )

    def build_bias(head, carry):
        tile = jnp.broadcast_to(lines[pl.ds(head, 1), :], (length, span))
        tile = pltpu.roll(tile, length + 1, 1, stride=1, stride_axis=0)
        for chunk in range(chunks):
            bias[
                chunk,
                head // per_tile,
                :,
                pl.ds(pl.multiple_of(head % per_tile * length, length), length),
            ] = tile[chunk * rows : (chunk + 1) * rows, :length]
        return carry

    lax.fori_loop(0, heads, build_bias, 0)
    gain_local.wait()

    @pl.when(home)
    def _():
        own_local.wait()

    def gain_wait(step, carry):
        gain_arrival((me + step) % count).wait_recv()
        return carry

    lax.fori_loop(1, count, gain_wait, 0)
    gain_half = gains[
        pl.ds(0, 8), pl.ds(pl.multiple_of(row * half, half), half)
    ][0:1, :].astype(jnp.float32)

    def multiply_gain(seq, start, size):
        values = xs[seq, pl.ds(start, size), :].astype(jnp.float32)
        scaled[pl.ds(start, size), :] = (values * gain_half).astype(jnp.bfloat16)
        return jnp.sum(values * values, axis=1, keepdims=True)

    def outgoing(chunk):
        squares = multiply_gain(1 - row, chunk * half_rows, half_rows)
        for start in range(0, half_rows, 128):
            sums_out[chunk, :, start : start + 128] = jnp.broadcast_to(
                squares[start : start + 128], (128, 128)
            ).T[0:8]
        sum_copy(chunk).start()

        def turn(group, carry):
            columns = pl.ds(pl.multiple_of(group * group_width, group_width), group_width)
            for index in range(3):
                part_out[chunk, group, :, pl.ds(index * group_width, group_width)] = jnp.dot(
                    scaled[pl.ds(chunk * half_rows, half_rows), :],
                    qkv[pl.ds(index * half, half), columns],
                    preferred_element_type=jnp.float32,
                ).astype(jnp.bfloat16)
            part_copy(chunk, group).start()
            return carry

        lax.fori_loop(0, groups, turn, 0)

    def fan(piece):
        wo_y_arrival(piece).wait_recv()
        for flip in (1, 2, 3):
            wo_fan(flip, piece, lane).start()

    token_spread(True, 0)
    launch(False, 0)
    fan(0)
    token_spread(False, 0)
    launch(False, 1)
    for load in loads:
        load.wait()
    fan(1)
    outgoing(0)
    token_spread(False, 1)
    launch(True, 1)
    fan(2)
    outgoing(1)
    fan(3)
    token_spread(True, 1)
    own_squares = multiply_gain(row, 0, length)
    for chunk in range(halves):
        sum_copy(chunk).wait_recv()
    other_squares = jnp.concatenate(
        [
            jnp.broadcast_to(sums_in[chunk, 0:1, start : start + 128], (128, 128)).T[:, 0:1]
            for chunk in range(halves)
            for start in range(0, half_rows, 128)
        ]
    )
    scale = lax.rsqrt((own_squares + other_squares) / (count * width) + epsilon)
    members = 128 // head_size
    first_lanes = lax.broadcasted_iota(jnp.int32, (length, 128), 1)

    def bias_of(head):
        lanes = pl.ds(pl.multiple_of(head % per_tile * length, length), length)
        return jnp.concatenate(
            [bias[chunk, head // per_tile, :, lanes] for chunk in range(chunks)]
        )

    def attend(member_group, carry):
        columns = pl.ds(pl.multiple_of(member_group * group_width, group_width), group_width)
        products = [
            jnp.dot(scaled[...], qkv[pl.ds(index * half, half), columns], preferred_element_type=jnp.float32)
            for index in range(3)
        ]
        for chunk in range(halves):
            part_copy(chunk, member_group).wait_recv()
        query, key, value = [
            (
                (
                    product
                    + part_in[:, member_group, :, pl.ds(index * group_width, group_width)]
                    .astype(jnp.float32)
                    .reshape(length, group_width)
                )
                * scale
            ).astype(jnp.bfloat16)
            for index, product in enumerate(products)
        ]
        for tile in range(group_width // 128):
            cut = slice(tile * 128, (tile + 1) * 128)
            query_pair, key_pair, value_pair = query[:, cut], key[:, cut], value[:, cut]
            outcome = None
            for member in range(members):
                mask = jnp.logical_and(
                    first_lanes >= member * head_size, first_lanes < (member + 1) * head_size
                )
                scores = (
                    lax.dot_general(
                        jnp.where(mask, query_pair.astype(jnp.float32), 0.0).astype(jnp.bfloat16),
                        key_pair,
                        (((1,), (1,)), ((), ())),
                        preferred_element_type=jnp.float32,
                    )
                    + bias_of(member_group * (group_width // head_size) + tile * members + member)
                )
                exponent = jnp.exp(scores - jnp.max(scores, axis=1, keepdims=True))
                total = jnp.sum(exponent, axis=1, keepdims=True)
                mixed = jnp.dot(
                    (exponent / total).astype(jnp.bfloat16),
                    value_pair,
                    preferred_element_type=jnp.float32,
                )
                outcome = mixed if outcome is None else jnp.where(mask, mixed, outcome)
            att[
                :, pl.ds(pl.multiple_of(member_group * group_width + tile * 128, 128), 128)
            ] = outcome.astype(jnp.bfloat16)
        return carry

    lax.fori_loop(0, groups, attend, 0)

    later = [
        pltpu.make_async_copy(gate_ref, gate, d_sem.at[0]),
        pltpu.make_async_copy(up_ref, up, d_sem.at[1]),
        pltpu.make_async_copy(down_ref, down, d_sem.at[2]),
    ]
    later[0].start()
    later[1].start()
    wo_local.wait()
    for piece in range(pieces):
        for flip in (1, 2, 3):
            wo_fan(flip, piece, lane ^ flip).wait_recv()

    def project(block, carry):
        columns = pl.ds(pl.multiple_of(block * width, width), width)
        share[block] = jnp.dot(
            att[...], out_full[:, columns], preferred_element_type=jnp.float32
        ).astype(jnp.bfloat16)
        return carry

    lax.fori_loop(0, count, project, 0)
    for piece in range(pieces):
        wo_y(piece).wait_send()
        for flip in (1, 2, 3):
            wo_fan(flip, piece, lane).wait_send()
    later[2].start()

    def columns(block):
        return pl.ds(pl.multiple_of(block * width, width), width)

    def chunk_rows(chunk):
        return pl.ds(pl.multiple_of(chunk * rows, rows), rows)

    def hop(outs, ins, sends, recvs, chunk, block, rightward):
        slot = block if rightward else jnp.where(block == me - 1, count, block)
        return pltpu.make_async_remote_copy(
            src_ref=outs.at[chunk, block],
            dst_ref=ins.at[chunk, slot],
            send_sem=sends.at[chunk, block],
            recv_sem=recvs.at[chunk, slot],
            device_id={"ma": me + 1 if rightward else me - 1},
            device_id_type=MESH,
        )

    def landed(outs, ins, sends, recvs, chunk, slot, from_left):
        return pltpu.make_async_remote_copy(
            src_ref=outs.at[chunk, 0],
            dst_ref=ins.at[chunk, slot],
            send_sem=sends.at[chunk, 0],
            recv_sem=recvs.at[chunk, slot],
            device_id={"ma": me - 1 if from_left else me + 1},
            device_id_type=MESH,
        )

    def across(chunk, block):
        return pltpu.make_async_remote_copy(
            src_ref=y_out.at[chunk, block],
            dst_ref=y_in.at[chunk, block],
            send_sem=a_send.at[chunk, block],
            recv_sem=a_recv.at[chunk, block],
            device_id={"row": 1 - row},
            device_id_type=MESH,
        )

    def spot(chunk, seq, block):
        return group.at[chunk, seq, :, columns(block)]

    def pass_on(way, chunk, block):
        here = spot(chunk, row, block)
        return pltpu.make_async_remote_copy(
            src_ref=here,
            dst_ref=here,
            send_sem=d_send.at[way, chunk, block],
            recv_sem=d_recv.at[chunk, block],
            device_id={"ma": me + 1 - 2 * way},
            device_id_type=MESH,
        )

    def cross(chunk, seq, block):
        here = spot(chunk, seq, block)
        return pltpu.make_async_remote_copy(
            src_ref=here,
            dst_ref=here,
            send_sem=x_send.at[chunk, block],
            recv_sem=x_recv.at[chunk, block],
            device_id={"row": 1 - row},
            device_id_type=MESH,
        )

    middle = count // 2

    def crosses(block):
        return jnp.logical_not(
            jnp.logical_or(
                jnp.logical_and(block == 0, me >= middle),
                jnp.logical_and(block == count - 1, me < middle),
            )
        )

    def relay(end, chunk):
        here = spot(chunk, 1 - row, end * (count - 1))
        return pltpu.make_async_remote_copy(
            src_ref=here,
            dst_ref=here,
            send_sem=r_send.at[end, chunk],
            recv_sem=r_recv.at[end, chunk],
            device_id={"ma": me + 1 - 2 * end},
            device_id_type=MESH,
        )

    def relay_turn(end):
        return me - (middle - 1) if end == 0 else middle - me

    def relays(end):
        turn = relay_turn(end)
        return jnp.logical_and(turn >= 0, turn < middle)

    def residual(chunk):
        group[chunk, row, :, columns(me)] = (
            tok_ref[chunk_rows(chunk), :].astype(jnp.float32) + total[...]
        ).astype(jnp.bfloat16)
        cross(chunk, row, me).start()

        @pl.when(me < count - 1)
        def _():
            pass_on(0, chunk, me).start()

        @pl.when(me > 0)
        def _():
            pass_on(1, chunk, me).start()

    def encode(chunk):
        out_ref[chunk_rows(chunk), :] = (
            group[chunk, row, :, columns(me)].astype(jnp.float32) + total[...]
        ).astype(jnp.bfloat16)

    attention_line = (c_out, c_in, c_send, c_recv)
    hidden_line = (c_out, e_in, e_send, e_recv)

    def chain(line, chunk, step, last):
        outs, ins, sends, recvs = line
        for rightward in (True, False):
            block = me + step if rightward else me - step
            inside = jnp.logical_and(block >= 0, block < count)
            if not rightward:
                inside = jnp.logical_and(inside, step > 0)

            @pl.when(inside)
            def _():
                if last:
                    across(chunk, block).wait_recv()
                    total[...] = kept[chunk, block] + y_in[chunk, block].astype(jnp.float32)
                else:
                    total[...] = share[block, chunk_rows(chunk), :].astype(jnp.float32)

                if rightward:

                    @pl.when(me > 0)
                    def _():
                        landed(*line, chunk, block, True).wait_recv()
                        total[...] = total[...] + ins[chunk, block].astype(jnp.float32)

                    @pl.when(jnp.logical_and(step == 0, me < count - 1))
                    def _():
                        landed(*line, chunk, count, False).wait_recv()
                        total[...] = total[...] + ins[chunk, count].astype(jnp.float32)

                    @pl.when(step == 0)
                    def _():
                        if last:
                            encode(chunk)
                        else:
                            residual(chunk)

                    @pl.when(step > 0)
                    def _():
                        if last:
                            hop(*attention_line, chunk, block, True).wait_send()
                        outs[chunk, block] = total[...].astype(jnp.bfloat16)
                        hop(*line, chunk, block, True).start()

                else:

                    @pl.when(me < count - 1)
                    def _():
                        landed(*line, chunk, block, False).wait_recv()
                        total[...] = total[...] + ins[chunk, block].astype(jnp.float32)

                    if last:
                        hop(*attention_line, chunk, block, False).wait_send()
                    outs[chunk, block] = total[...].astype(jnp.bfloat16)
                    hop(*line, chunk, block, False).start()

    def spread(chunk, step):
        for way in (0, 1):
            block = me - step if way == 0 else me + step

            @pl.when(jnp.logical_and(block >= 0, block < count))
            def _():
                pass_on(way, chunk, block).wait_recv()

                @pl.when(crosses(block))
                def _():
                    cross(chunk, row, block).start()

                @pl.when(me < count - 1 if way == 0 else me > 0)
                def _():
                    pass_on(way, chunk, block).start()

    tile = min(256, hidden.shape[1])
    norm_rows = 16

    def feed(batch):
        def arrive(index, carry):
            chunk = batch * per + index // count
            block = index % count
            first = block == 0
            final = block == count - 1
            taken = jnp.logical_or(
                jnp.logical_and(first, relays(0)), jnp.logical_and(final, relays(1))
            )

            @pl.when(jnp.logical_and(crosses(block), jnp.logical_not(taken)))
            def _():
                cross(chunk, 1 - row, block).wait_recv()

            for end in (0, 1):

                @pl.when(
                    jnp.logical_and(
                        final if end else first,
                        jnp.logical_not(jnp.logical_or(crosses(block), taken)),
                    )
                )
                def _():
                    relay(end, chunk).wait_recv()

            return carry

        lax.fori_loop(0, per * count, arrive, 0)
        strips = rows // norm_rows

        def normalize(index, carry):
            slab = index // strips
            start = pl.multiple_of(index % strips * norm_rows, norm_rows)
            values = group[
                batch * per + slab // 2, slab % 2, pl.ds(start, norm_rows), :
            ].astype(jnp.float32)
            mean_square = jnp.mean(values * values, axis=1, keepdims=True)
            normed[pl.ds(pl.multiple_of(index * norm_rows, norm_rows), norm_rows), :] = (
                values
                * lax.rsqrt(mean_square + epsilon)
                * gains[8:9, :].astype(jnp.float32)
            ).astype(jnp.bfloat16)
            return carry

        lax.fori_loop(0, 2 * per * strips, normalize, 0)

        @pl.when(batch == 0)
        def _():
            for load in later:
                load.wait()

        def gated(index, carry):
            cut = pl.ds(pl.multiple_of(index * tile, tile), tile)
            gate_act = jnp.dot(normed[...], gate[:, cut], preferred_element_type=jnp.float32)
            up_act = jnp.dot(normed[...], up[:, cut], preferred_element_type=jnp.float32)
            hidden[:, cut] = (jax.nn.gelu(gate_act, approximate=True) * up_act).astype(
                jnp.bfloat16
            )
            return carry

        lax.fori_loop(0, hidden.shape[1] // tile, gated, 0)

        def contract(index, carry):
            step = count - 1 - index // 2
            rightward = index % 2 == 0
            block = jnp.where(rightward, me + step, me - step)
            inside = jnp.logical_and(block >= 0, block < count)

            @pl.when(jnp.logical_and(inside, jnp.logical_or(step > 0, rightward)))
            def _():
                pair[...] = jnp.dot(
                    hidden[...], down[:, columns(block)], preferred_element_type=jnp.float32
                ).reshape(per, 2, rows, width)
                for sub in range(per):
                    chunk = batch * per + sub
                    y_out[chunk, block] = pair[sub, 1 - row].astype(jnp.bfloat16)
                    across(chunk, block).start()
                    kept[chunk, block] = pair[sub, row]

            return carry

        lax.fori_loop(0, 2 * count, contract, 0)

    def tick(time, carry):
        def active(since):
            return jnp.logical_and(
                since % spacing == 0, jnp.logical_and(since >= 0, since < spacing * chunks)
            )

        def attention_turn(index, inner):
            since = time - (count - 1) + index

            @pl.when(active(since))
            def _():
                chain(attention_line, since // spacing, index, False)

            return inner

        def spread_turn(index, inner):
            hop_index = count - 1 - index
            since = time - (count - 1) - hop_index

            @pl.when(active(since))
            def _():
                spread(since // spacing, hop_index)

            return inner

        def hidden_turn(index, inner):
            since = time - hidden_base - (count - 1) + index

            @pl.when(active(since))
            def _():
                chain(hidden_line, since // spacing, index, True)

            return inner

        def relay_all():
            for end in (0, 1):
                turn = relay_turn(end)
                since = time - relay_base - turn
                chunk = since // spacing

                @pl.when(jnp.logical_and(relays(end), active(since)))
                def _():
                    @pl.when(turn == 0)
                    def _():
                        cross(chunk, 1 - row, end * (count - 1)).wait_recv()

                    @pl.when(turn > 0)
                    def _():
                        relay(end, chunk).wait_recv()

                    relay(end, chunk).start()

        def feed_turn():
            since = time - feed_base

            @pl.when(
                jnp.logical_and(
                    since % (spacing * per) == 0,
                    jnp.logical_and(since >= 0, since < spacing * chunks),
                )
            )
            def _():
                feed(since // (spacing * per))

        lax.fori_loop(0, count - 1, spread_turn, 0)
        lax.fori_loop(0, count, hidden_turn, 0)
        lax.fori_loop(0, count, attention_turn, 0)
        relay_all()
        feed_turn()
        return carry

    feed_base = 2 * count
    hidden_base = feed_base + 1
    relay_base = 2 * count - middle
    lax.fori_loop(0, spacing * (chunks - 1) + hidden_base + count, tick, 0)

    def drain(index, carry):
        chunk = index // count
        block = index % count
        across(chunk, block).wait_send()

        @pl.when(crosses(block))
        def _():
            cross(chunk, row, block).wait_send()

        for end in (0, 1):

            @pl.when(jnp.logical_and(block == end, relays(end)))
            def _():
                relay(end, chunk).wait_send()

        @pl.when(block > me)
        def _():
            hop(*hidden_line, chunk, block, True).wait_send()

        @pl.when(block < me)
        def _():
            hop(*hidden_line, chunk, block, False).wait_send()

        @pl.when(jnp.logical_and(me < count - 1, block <= me))
        def _():
            pass_on(0, chunk, block).wait_send()

        @pl.when(jnp.logical_and(me > 0, block >= me))
        def _():
            pass_on(1, chunk, block).wait_send()

        return carry

    lax.fori_loop(0, chunks * count, drain, 0)


    for chunk in range(halves):
        sum_copy(chunk).wait_send()

        def part_drain(group, carry):
            part_copy(chunk, group).wait_send()
            return carry

        lax.fori_loop(0, groups, part_drain, 0)

        @pl.when(jnp.logical_not(home))
        def _():
            y_copy(chunk).wait_send()

        def z_drain(slot, carry):
            block = slot + row * half_blocks
            for seq in (0, 1):

                @pl.when(jnp.logical_and(me < count - 1, block <= me))
                def _():
                    z_copy(0, seq, chunk, block).wait_send()

                @pl.when(jnp.logical_and(me > 0, block >= me))
                def _():
                    z_copy(1, seq, chunk, block).wait_send()

            return carry

        lax.fori_loop(0, half_blocks, z_drain, 0)

    def gain_drain(offset, carry):
        gain_copy(offset).wait_send()
        return carry

    lax.fori_loop(1, count, gain_drain, 0)


def layer(
    tok, attn_gain, ffn_gain, table, wq, wk, wv, wo, gate, up, down, count, collective_id
):
    length, width = tok.shape
    halves, chunks, per, spacing, pieces = 2, 4, 1, 2, 4
    inner = wq.shape[1]
    heads = table.shape[0]
    groups = max(1, inner // 256)
    half = wq.shape[0]
    half_rows = length // halves
    rows = length // chunks
    group_width = inner // groups
    per_tile = max(1, min(heads, width // length))
    dma = pltpu.SemaphoreType.DMA
    vmem = pl.BlockSpec(memory_space=pltpu.VMEM)
    anywhere = pl.BlockSpec(memory_space=pl.ANY)
    bf16 = lambda *shape: pltpu.VMEM(shape, jnp.bfloat16)
    f32 = lambda *shape: pltpu.VMEM(shape, jnp.float32)
    bias_shape = (chunks, heads // per_tile, rows, per_tile * length)
    kept_shape = (chunks, count, rows, width)
    shared = bias_shape == kept_shape

    def body(*refs):
        refs = list(refs)
        if shared:
            refs.insert(31, refs[30])
        layer_kernel(count, halves, groups, chunks, per, spacing, *refs)

    return pl.pallas_call(
        body,
        out_shape=jax.ShapeDtypeStruct((length, width), jnp.bfloat16),
        in_specs=[vmem] * 4 + [anywhere] * 7,
        out_specs=vmem,
        scratch_shapes=[
            bf16(3 * half, inner),
            bf16(*up.shape),
            bf16(wo.shape[0], 2 * wo.shape[1]),
            bf16(16, count * width),
            bf16(2, length, half),
            bf16(length, half),
            bf16(halves, groups, half_rows, 3 * group_width),
            bf16(halves, groups, half_rows, 3 * group_width),
            f32(halves, 8, half_rows),
            f32(halves, 8, half_rows),
            f32(heads, 2 * length),
            bf16(16, width),
            bf16(length, inner),
            bf16(count, length, width),
            bf16(chunks, 2, rows, count * width),
            bf16(2 * per * rows, count * width),
            bf16(2 * per * rows, down.shape[0]),
            f32(per, 2, rows, width),
            f32(*bias_shape),
        ]
        + ([] if shared else [f32(*kept_shape)])
        + [
            f32(rows, width),
            bf16(chunks, count, rows, width),
            bf16(chunks, count + 1, rows, width),
            bf16(chunks, count + 1, rows, width),
            bf16(chunks, count, rows, width),
            bf16(chunks, count, rows, width),
            dma((3,)),
            dma((3,)),
            dma,
            dma,
            dma,
            dma((count,)),
            dma((count,)),
            dma((halves,)),
            dma((halves,)),
            dma((2, 2, halves, count // 2)),
            dma((2, halves, count // 2)),
            dma((halves, groups)),
            dma((halves, groups)),
            dma((halves,)),
            dma((halves,)),
            dma((pieces,)),
            dma((pieces,)),
            dma((3, pieces)),
            dma((3, pieces)),
            dma((chunks, count)),
            dma((chunks, count + 1)),
            dma((chunks, count)),
            dma((chunks, count + 1)),
            dma((chunks, count)),
            dma((chunks, count)),
            dma((2, chunks, count)),
            dma((chunks, count)),
            dma((chunks, count)),
            dma((chunks, count)),
            dma((2, chunks)),
            dma((2, chunks)),
        ],
        compiler_params=pltpu.CompilerParams(
            collective_id=collective_id, has_side_effects=True, vmem_limit_bytes=67043328
        ),
    )(tok, attn_gain, ffn_gain, table, wq, wk, wv, wo, gate, up, down)


def on_device(
    tokens,
    attn_gain,
    query_weight,
    key_weight,
    value_projection_matrix,
    attention_output_matrix,
    bucket_bias_matrix,
    ffn_gain,
    gate_weight,
    up_weight,
    down_projection_weight,
):
    sequences, length, part_width = tokens.shape
    ma_count = lax.axis_size("ma")
    slab_rows = sequences * length
    token_rows = tokens.reshape(slab_rows, part_width)
    encoded = layer(
        token_rows,
        attn_gain,
        ffn_gain,
        bucket_bias_matrix.T,
        query_weight,
        key_weight,
        value_projection_matrix,
        attention_output_matrix,
        gate_weight,
        up_weight,
        down_projection_weight,
        ma_count,
        1,
    )
    return encoded.reshape(sequences, length, part_width)


def solution(mesh):
    in_specs = (
        P(("ba", "row"), None, "ma"),
        P("ma"),
        P("row", "ma"),
        P("row", "ma"),
        P("row", "ma"),
        P("ma", "row"),
        P(None, "ma"),
        P("ma"),
        P(None, ("ma", "row")),
        P(None, ("ma", "row")),
        P(("ma", "row"), None),
    )
    out_specs = P(("ba", "row"), None, "ma")
    return jax.shard_map(
        on_device, mesh=mesh, in_specs=in_specs, out_specs=out_specs, check_vma=False
    )
```
